32 devices in a mesh: py: 4 (over z), px: 8 (over y, x, core).
Axes of the slice: x: 2, y: 2, z: 4, core: 2. Of those that a mesh axis runs over, the one named last changes fastest.
Arguments:
- residual: bfloat16 [4, 8, 4096, 128], P('py', 'px'), may hold values from -10 to 75
- footprints: bfloat16 [4, 8, 40, 4096], P('py', 'px'), may hold values from 0.049804688 to 1
- traces: bfloat16 [4, 8, 40, 128], P('py', 'px'), may hold values from 0.099609375 to 2
- merge_pairs: int32 [4, 8, 16, 3], P('py', 'px'), may hold values from 0 to 39, as said below
- pair_counts: int32 [4, 8], P('py', 'px'), may hold values from 1 to 16, as said below
- comp_counts: int32 [4, 8], P('py', 'px'), may hold values from 27 to 40, as said below
- row_intersections: int32 [3], replicated, may hold values from 8 to 24
- col_intersections: int32 [7], replicated, may hold values from 8 to 24
Outputs:
- new_footprints: bfloat16 [4, 8, 40, 4096], P('py', 'px')
- new_traces: bfloat16 [4, 8, 40, 128], P('py', 'px')
- correlations: float32 [4, 8, 40, 24], P('py', 'px')
The draws below stay inside these ranges and needn't reach their ends.
Inputs may be any that keep to these rules, and one draw needn't show every extreme that they name: `merge_pairs`: in slot m < pair_counts[p]: a component id i with 24 <= i < comp_counts[p], a direction d whose neighbour patch exists, and a slot s < 3; ids and (d, s) are distinct within a patch. Later slots are unused. `pair_counts`: at most 3 times the number of neighbours of the patch; some patch has 16. `comp_counts`: at least 24 + pair_counts[p]; components from comp_counts[p] on are unused; some patch has 40.
All inputs are finite; a program needn't handle non-finite values.
Results may differ from the reference program's by a relative error of at most 0.0026.
Values may be sent and summed in bfloat16 or wider, within the bound.
A program may use at most 64 MiB of HBM per device.

```python
import math
import jax
import jax.numpy as jnp
from jax import lax

PH = 64
PW = 64
K = 40
NBR = 3
BORDER = 24
MP = 16
F = 128
ITERS = 4
OV_LO = 8
OV_HI = 24
GR = 4
GC = 8


def merge_layout(key):
    base_key = jax.random.fold_in(key, 7211)
    key_counts, key_codes, key_extra, key_owned = jax.random.split(base_key, 4)
    grid_row = jnp.arange(GR, dtype=jnp.int32)[:, None] + jnp.zeros((1, GC), jnp.int32)
    grid_col = jnp.arange(GC, dtype=jnp.int32)[None, :] + jnp.zeros((GR, 1), jnp.int32)
    direction = jnp.arange(8, dtype=jnp.int32)
    flat_index = direction + (direction >= 4).astype(jnp.int32)
    step_y = flat_index // 3 - 1
    step_x = flat_index % 3 - 1
    target_y = grid_row[:, :, None] + step_y
    target_x = grid_col[:, :, None] + step_x
    present = (target_y >= 0) & (target_y < GR) & (target_x >= 0) & (target_x < GC)
    capacity = jnp.minimum(NBR * jnp.sum(present.astype(jnp.int32), axis=-1), MP)
    divisor = 1 + jax.random.randint(key_counts, (GR, GC), 0, 4)
    pair_total = 1 + (capacity - 1) // divisor
    pair_total = jnp.where((grid_row == 1) & (grid_col == 1), capacity, pair_total)
    code_index = jnp.arange(BORDER, dtype=jnp.int32)
    code_present = jnp.repeat(present, NBR, axis=-1)
    code_scores = jax.random.randint(key_codes, (GR, GC, BORDER), 0, 1 << 20) * BORDER + code_index + jnp.where(code_present, 0, 1 << 26)
    chosen = jnp.argsort(code_scores, axis=-1)[:, :, :MP].astype(jnp.int32)
    extra_count = jax.random.randint(key_extra, (GR, GC), 0, K - BORDER - pair_total + 1)
    component_total = BORDER + pair_total + extra_count
    spare_index = jnp.arange(K - BORDER, dtype=jnp.int32)
    owned_scores = jax.random.randint(key_owned, (GR, GC, K - BORDER), 0, 1 << 20) * (K - BORDER) + spare_index + jnp.where(BORDER + spare_index[None, None, :] < component_total[:, :, None], 0, 1 << 26)
    owned_ids = BORDER + jnp.argsort(owned_scores, axis=-1)[:, :, :MP].astype(jnp.int32)
    pair_table = jnp.stack([owned_ids, chosen // NBR, chosen % NBR], axis=-1).astype(jnp.int32)
    return (pair_table, pair_total.astype(jnp.int32), component_total.astype(jnp.int32))


def draw_merge_pairs(key, part):
    return merge_layout(key)[0]


def draw_pair_counts(key, part):
    return merge_layout(key)[1]


def draw_comp_counts(key, part):
    return merge_layout(key)[2]


def rank_mask(key, count, chosen):
    scores = jax.random.randint(key, (GR, GC, count), 0, 1 << 30)
    ranks = jnp.argsort(jnp.argsort(scores, axis=-1), axis=-1)
    return (ranks < chosen).astype(jnp.float32)


def draw_residual(key, part):
    base_key = jax.random.fold_in(key, 5309)
    key_noise, key_pixels, key_frames, key_spatial, key_temporal = jax.random.split(base_key, 5)
    pixel_count = PH * PW
    pixel_live = max(pixel_count // 32, 1)
    frame_live = max(F // 16, 1)
    pixel_mask = rank_mask(key_pixels, pixel_count, pixel_live)
    frame_mask = rank_mask(key_frames, F, frame_live)
    spatial = jnp.exp(jax.random.uniform(key_spatial, (GR, GC, pixel_count), jnp.float32, math.log(0.05), 0.0)) * pixel_mask
    temporal = jnp.exp(jax.random.uniform(key_temporal, (GR, GC, F), jnp.float32, math.log(0.1), math.log(2.0))) * frame_mask
    noise = jnp.clip(2.0 * jax.random.normal(key_noise, (GR, GC, pixel_count, F), jnp.float32), -10.0, 10.0)
    strength = 1.2
    amplitude = strength * math.sqrt(pixel_count * F / (pixel_live * frame_live))
    values = noise + amplitude * spatial[:, :, :, None] * temporal[:, :, None, :]
    return values.astype(jnp.bfloat16)


def with_ends(values, rng, smallest, largest):
    shape = values.shape
    index_at = [jax.random.randint(jax.random.fold_in(rng, axis), (), 0, shape[axis]) for axis in range(len(shape))]
    values = values.at[tuple(index_at)].set(smallest)
    longest = shape.index(max(shape))
    index_at[longest] = (index_at[longest] + 1) % shape[longest]
    return values.at[tuple(index_at)].set(largest)


def block_scale(own_key, shape, cuts, least, top_value):
    def one(position, shards_of):
        heights = jax.random.uniform(jax.random.fold_in(jax.random.fold_in(own_key, 6), position), (shards_of,), jnp.float32, least / len(cuts), top_value / len(cuts))
        return jnp.repeat(jnp.exp(heights), shape[position] // shards_of).reshape((-1,) + (1,) * (len(shape) - position - 1))

    factor_of = one(*cuts[0])
    for cut in cuts[1:]:
        factor_of = factor_of * one(*cut)
    return factor_of


def setup_inputs(seed: int = 0) -> dict:
    splits = jax.random.split(jax.random.key(seed), 9)
    residual = draw_residual(jax.random.fold_in(splits[8], 71), 0)
    footprints = jnp.clip(jnp.exp(math.log(1.0) - 2.9996462 * jax.random.uniform(splits[1], (GR, GC, K, PH * PW), jnp.float32) ** block_scale(splits[1], (GR, GC, K, PH * PW), ((0, 4), (1, 8)), -0.2, 0.2)), 0.049804688, 1.0).astype(jnp.bfloat16)
    traces = jnp.clip(jnp.exp(math.log(2.0) - 2.9996462 * jax.random.uniform(splits[2], (GR, GC, K, F), jnp.float32) ** block_scale(splits[2], (GR, GC, K, F), ((0, 4), (1, 8)), -0.2, 0.2)), 0.099609375, 2.0).astype(jnp.bfloat16)
    merge_pairs = draw_merge_pairs(jax.random.fold_in(splits[8], 71), 0)
    pair_counts = draw_pair_counts(jax.random.fold_in(splits[8], 71), 0)
    comp_counts = draw_comp_counts(jax.random.fold_in(splits[8], 71), 0)
    row_intersections = jax.random.randint(splits[6], (GR - 1,), OV_LO, OV_HI + 1).astype(jnp.int32)
    col_intersections = with_ends(jax.random.randint(splits[7], (GC - 1,), OV_LO, OV_HI + 1), jax.random.fold_in(splits[7], 1), OV_LO, OV_HI).astype(jnp.int32)
    return {"residual": residual, "footprints": footprints, "traces": traces, "merge_pairs": merge_pairs, "pair_counts": pair_counts, "comp_counts": comp_counts, "row_intersections": row_intersections, "col_intersections": col_intersections}


epsilon = 1e-05

def direction_steps(direction):
    flat_index = direction + (direction >= 4).astype(jnp.int32)
    return (flat_index // 3 - 1, flat_index % 3 - 1)

def lookup_table(table, index):
    places = jnp.arange(table.shape[0], dtype=jnp.int32)
    return lax.optimization_barrier(jnp.sum(jnp.where(places[None, :] == index[:, None], table[None, :], 0), axis=1)).astype(jnp.int32)

def pair_offsets(direction, grid_row, grid_col, row_intersections, col_intersections):
    step_y, step_x = direction_steps(direction)
    band_y = jnp.clip(grid_row + jnp.minimum(step_y, 0), 0, row_intersections.shape[0] - 1)
    band_x = jnp.clip(grid_col + jnp.minimum(step_x, 0), 0, col_intersections.shape[0] - 1)
    shift_y = step_y * (PH - lookup_table(row_intersections, band_y))
    shift_x = step_x * (PW - lookup_table(col_intersections, band_x))
    return (shift_y, shift_x)

def move_pixels(values, shift_y, shift_x, filler):
    pixels = jnp.arange(PH * PW, dtype=jnp.int32)
    source_y = pixels[None, :] // PW - shift_y[:, None]
    source_x = pixels[None, :] % PW - shift_x[:, None]
    inside = (source_y >= 0) & (source_y < PH) & (source_x >= 0) & (source_x < PW)
    source = jnp.clip(source_y, 0, PH - 1) * PW + jnp.clip(source_x, 0, PW - 1)
    taken = jnp.take_along_axis(values, source, axis=1)
    return jnp.where(inside, taken, filler)

def refit_pairs(residue, own_footprints, own_traces, pair_table, pair_total, border, grid_row, grid_col, row_intersections, col_intersections):
    pixel_count = PH * PW
    owned_ids = pair_table[:, 0]
    direction = pair_table[:, 1]
    border_index = NBR * direction + pair_table[:, 2]
    in_use = jnp.arange(MP, dtype=jnp.int32) < pair_total
    a_own = jnp.take(own_footprints, owned_ids, axis=0).astype(jnp.float32)
    c_own = jnp.take(own_traces, owned_ids, axis=0).astype(jnp.float32)
    remote = jnp.take(border, border_index, axis=0)
    a_remote_raw = remote[:, :pixel_count].astype(jnp.float32)
    c_remote = remote[:, pixel_count:].astype(jnp.float32)
    shift_y, shift_x = pair_offsets(direction, grid_row, grid_col, row_intersections, col_intersections)
    a_remote = move_pixels(a_remote_raw, shift_y, shift_x, 0.0)
    trace_now = c_own
    shape_now = a_own
    for iteration in range(ITERS):
        across = jnp.dot(trace_now.astype(jnp.bfloat16), residue.T, preferred_element_type=jnp.float32)
        across = across + a_own * lax.optimization_barrier(jnp.sum(c_own * trace_now, axis=1, keepdims=True)) + a_remote * lax.optimization_barrier(jnp.sum(c_remote * trace_now, axis=1, keepdims=True))
        shape_now = jnp.maximum(across, 0.0) / (lax.optimization_barrier(jnp.sum(trace_now * trace_now, axis=1, keepdims=True)) + epsilon * F)
        downward = jnp.dot(shape_now.astype(jnp.bfloat16), residue, preferred_element_type=jnp.float32)
        downward = downward + c_own * lax.optimization_barrier(jnp.sum(a_own * shape_now, axis=1, keepdims=True)) + c_remote * lax.optimization_barrier(jnp.sum(a_remote * shape_now, axis=1, keepdims=True))
        trace_now = jnp.maximum(downward, 0.0) / (lax.optimization_barrier(jnp.sum(shape_now * shape_now, axis=1, keepdims=True)) + epsilon * pixel_count)
    footprint_out = shape_now.astype(jnp.bfloat16)
    trace_out = trace_now.astype(jnp.bfloat16)
    remote_new = move_pixels(footprint_out.astype(jnp.float32), -shift_y, -shift_x, a_remote_raw).astype(jnp.bfloat16)
    owner_hot = ((owned_ids[None, :] == jnp.arange(K, dtype=jnp.int32)[:, None]) & in_use[None, :]).astype(jnp.float32)
    owner_hit = lax.optimization_barrier(jnp.sum(owner_hot, axis=1)) > 0
    new_foot = jnp.where(owner_hit[:, None], jnp.dot(owner_hot, footprint_out.astype(jnp.float32), precision=lax.Precision.HIGHEST), own_footprints.astype(jnp.float32)).astype(jnp.bfloat16)
    new_trace = jnp.where(owner_hit[:, None], jnp.dot(owner_hot, trace_out.astype(jnp.float32), precision=lax.Precision.HIGHEST), own_traces.astype(jnp.float32)).astype(jnp.bfloat16)
    border_hot = ((border_index[None, :] == jnp.arange(BORDER, dtype=jnp.int32)[:, None]) & in_use[None, :]).astype(jnp.float32)
    border_hit = lax.optimization_barrier(jnp.sum(border_hot, axis=1)) > 0
    sending = jnp.concatenate([remote_new, trace_out], axis=1).astype(jnp.float32)
    outgoing = jnp.where(border_hit[:, None], jnp.dot(border_hot, sending, precision=lax.Precision.HIGHEST), border.astype(jnp.float32)).astype(jnp.bfloat16)
    return (new_foot, new_trace, outgoing)

def neighbour_rows(block):
    padded = jnp.pad(block, ((1, 1), (1, 1), (0, 0), (0, 0)))
    pieces = []
    for direction in range(8):
        flat_index = direction + (1 if direction >= 4 else 0)
        step_y = flat_index // 3 - 1
        step_x = flat_index % 3 - 1
        source = NBR * (7 - direction)
        pieces.append(padded[1 + step_y:1 + step_y + GR, 1 + step_x:1 + step_x + GC, source:source + NBR])
    return jnp.concatenate(pieces, axis=2)

def neighbour_exists(grid_row, grid_col):
    flags = []
    for direction in range(8):
        flat_index = direction + (1 if direction >= 4 else 0)
        target_y = grid_row + flat_index // 3 - 1
        target_x = grid_col + flat_index % 3 - 1
        flags.append((target_y >= 0) & (target_y < GR) & (target_x >= 0) & (target_x < GC))
    return jnp.repeat(jnp.stack(flags, axis=-1), NBR, axis=-1)

def reference(residual, footprints, traces, merge_pairs, pair_counts, comp_counts, row_intersections, col_intersections):
    pixel_count = PH * PW
    patches = GR * GC
    packed = jnp.concatenate([footprints[:, :, :BORDER], traces[:, :, :BORDER]], axis=3)
    border = neighbour_rows(packed)
    local = traces.astype(jnp.float32)
    local = local - lax.optimization_barrier(jnp.mean(local, axis=-1, keepdims=True))
    remote = border[:, :, :, pixel_count:].astype(jnp.float32)
    remote = remote - lax.optimization_barrier(jnp.mean(remote, axis=-1, keepdims=True))
    covariance = jnp.einsum('rckf,rcbf->rckb', local, remote, precision=lax.Precision.HIGHEST) / F
    spread_local = lax.optimization_barrier(jnp.mean(local * local, axis=-1))
    spread_remote = lax.optimization_barrier(jnp.mean(remote * remote, axis=-1))
    correlation = covariance / jnp.sqrt((spread_local[..., :, None] + epsilon) * (spread_remote[..., None, :] + epsilon))
    flat_rows = jnp.arange(patches, dtype=jnp.int32) // GC
    flat_cols = jnp.arange(patches, dtype=jnp.int32) % GC

    def one_patch(items):
        residue, own_footprints, own_traces, pair_table, pair_total, border_block, grid_row, grid_col = items
        return refit_pairs(residue, own_footprints, own_traces, pair_table, pair_total, border_block, grid_row, grid_col, row_intersections, col_intersections)
    new_foot, new_trace, outgoing = lax.map(one_patch, (residual.reshape(patches, pixel_count, F), footprints.reshape(patches, K, pixel_count), traces.reshape(patches, K, F), merge_pairs.reshape(patches, MP, 3), pair_counts.reshape(patches), border.reshape(patches, BORDER, pixel_count + F), flat_rows, flat_cols))
    returned = neighbour_rows(outgoing.reshape(GR, GC, BORDER, pixel_count + F))
    new_foot = new_foot.reshape(GR, GC, K, pixel_count)
    new_trace = new_trace.reshape(GR, GC, K, F)
    grid_row = jnp.arange(GR, dtype=jnp.int32)[:, None] + jnp.zeros((1, GC), jnp.int32)
    grid_col = jnp.arange(GC, dtype=jnp.int32)[None, :] + jnp.zeros((GR, 1), jnp.int32)
    exists = neighbour_exists(grid_row, grid_col)
    reserved_foot = jnp.where(exists[..., None], returned[..., :pixel_count], new_foot[:, :, :BORDER])
    reserved_trace = jnp.where(exists[..., None], returned[..., pixel_count:], new_trace[:, :, :BORDER])
    alive = jnp.arange(K, dtype=jnp.int32)[None, None, :] < comp_counts[..., None]
    zero_value = jnp.zeros((), jnp.bfloat16)
    new_footprints = jnp.where(alive[..., None], jnp.concatenate([reserved_foot, new_foot[:, :, BORDER:]], axis=2), zero_value)
    new_traces = jnp.where(alive[..., None], jnp.concatenate([reserved_trace, new_trace[:, :, BORDER:]], axis=2), zero_value)
    correlations = jnp.where(alive[..., None], correlation, 0.0)
    return (new_footprints, new_traces, correlations)
```

```python
import functools

import jax
import jax.numpy as jnp
from jax import lax
from jax.experimental import pallas as pl
from jax.experimental.pallas import tpu as pltpu
from jax.sharding import PartitionSpec as P

PH = 64
PW = 64
NBR = 3
OV_HI = 24
ITERS = 4
EPS = 1e-05

PAD = 4
STRIP = OV_HI * PW
CHUNK = 512
WIDE = 1024
LANES = 128
LOW = (PH - OV_HI) // 2
ORDER = (0, 2, 5, 7, 1, 6, 3, 4)
RECEIVE = (3, 4, 1, 6, 0, 2, 5, 7)
STEPS = [(-1, -1), (-1, 0), (-1, 1), (0, -1), (0, 1), (1, -1), (1, 0), (1, 1)]
BF = jnp.bfloat16
F32 = jnp.float32
MESH = pl.DeviceIdType.MESH


def lanes_in(direction, pixels):
    dy = STEPS[direction][0]
    if dy > 0:
        return (0, STRIP)
    if dy < 0:
        return (pixels - STRIP, STRIP)
    return (0, pixels)


def lanes_out(direction, pixels):
    return lanes_in(7 - direction, pixels)


def dot(a, b):
    return jnp.dot(a, b, preferred_element_type=F32)


def dot_t(a, b):
    return lax.dot_general(a, b, (((1,), (1,)), ((), ())), preferred_element_type=F32)


def iota(shape, dim):
    return lax.broadcasted_iota(jnp.int32, shape, dim)


def narrow(x):
    return functools.reduce(jnp.add, [x[:, b:b + LANES] for b in range(0, x.shape[1], LANES)])


def shift_of(direction, up, down, left, right):
    flat = direction + (direction >= 4).astype(jnp.int32)
    row = (flat >= 3).astype(jnp.int32) + (flat >= 6).astype(jnp.int32)
    dy = row - 1
    dx = flat - 3 * row - 1
    oy = jnp.where(dy < 0, up - PH, jnp.where(dy > 0, PH - down, 0))
    ox = jnp.where(dx < 0, left - PW, jnp.where(dx > 0, PW - right, 0))
    return oy, ox


def inside_of(oy, ox, first, count):
    pixel = iota((1, count), 1) + first
    y = (pixel >> 6) - oy
    x = (pixel & (PW - 1)) - ox
    return (y >= 0) & (y < PH) & (x >= 0) & (x < PW)


def kernel(
    rows, cols,
    res_hbm, foot_hbm, trace_hbm, pair_hbm, pair_count, comp_count, row_hbm, col_hbm,
    out_foot, out_trace, out_corr,
    res_ref, foot_ref, trace_ref, pair_ref, row_ref, col_ref, sem_in,
    send, recv1, recv2, wide, res_t,
    border, border_trace, back, back_trace, a_own, a_rem, shape, take, keep,
    sem_s, sem_r,
):
    pixels = foot_ref.shape[1]
    frames = trace_ref.shape[1]
    comps = foot_ref.shape[0]
    slots = pair_ref.shape[2]
    nb = 8 * NBR
    nbp = 8 * PAD
    my_r = lax.axis_index("py")
    my_c = lax.axis_index("px")

    def target(d):
        return (my_r + STEPS[d][0], my_c + STEPS[d][1])

    def exists(d):
        r, c = target(d)
        return (r >= 0) & (r < rows) & (c >= 0) & (c < cols)

    barrier = pltpu.get_barrier_semaphore()
    for d in range(8):
        @pl.when(exists(d))
        def _():
            pl.semaphore_signal(barrier, 1, device_id=target(d), device_id_type=MESH)
    fetches = [
        (trace_hbm, trace_ref),
        (row_hbm, row_ref), (col_hbm, col_ref),
        (foot_hbm.at[pl.ds(0, nb)], foot_ref.at[pl.ds(0, nb)]),
        (pair_hbm, pair_ref),
        (foot_hbm.at[pl.ds(nb, comps - nb)], foot_ref.at[pl.ds(nb, comps - nb)]),
        (res_hbm, res_ref),
    ]
    fetches = [pltpu.make_async_copy(a, b, sem_in.at[i]) for i, (a, b) in enumerate(fetches)]
    for fetch in fetches:
        fetch.start()

    def span1(d):
        return lanes_in(d, pixels)[1] + frames

    def remote(src, dst, d, phase):
        return pltpu.make_async_remote_copy(
            src, dst, sem_s.at[d], sem_r.at[phase, 7 - d],
            device_id=target(d), device_id_type=MESH)

    def copy1(d):
        part = pl.ds(0, span1(d))
        return remote(send.at[d, :, part], recv1.at[7 - d, :, part], d, 0)

    def copy2(d):
        width = lanes_in(d, pixels)[1]
        return remote(send.at[d, :, pl.ds(span1(d), width)], recv2.at[7 - d, :, pl.ds(0, width)], d, 1)

    def copy3(d):
        width = lanes_in(d, pixels)[1]
        return remote(send.at[d, :, pl.ds(span1(d) + width, frames)],
                      recv2.at[7 - d, :, pl.ds(width, frames)], d, 1)

    def both(d):
        part = pl.ds(0, span1(d))
        return remote(send.at[d, :, part], recv2.at[7 - d, :, part], d, 1)

    def all_sent(d):
        part = send.at[d, :, pl.ds(0, 2 * span1(d))]
        return remote(part, part, d, 1)

    j = iota((nbp, nb), 0)
    pick = (((j & (PAD - 1)) < NBR) & (iota((nbp, nb), 1) == NBR * (j >> 2) + (j & (PAD - 1)))).astype(BF)
    border[...] = jnp.zeros_like(border)
    border_trace[...] = jnp.zeros_like(border_trace)
    back[...] = jnp.zeros_like(back)
    back_trace[...] = jnp.zeros_like(back_trace)
    fetches[0].wait()
    own_traces = trace_ref[...]
    packed_traces = dot(pick, own_traces[0:nb])
    for d in range(8):
        width = lanes_in(d, pixels)[1]
        send[d, :, width:width + frames] = packed_traces[PAD * d:PAD * d + PAD].astype(BF)
    fetches[1].wait()
    fetches[2].wait()
    up = row_ref[jnp.clip(my_r - 1, 0, rows - 2)]
    down = row_ref[jnp.clip(my_r, 0, rows - 2)]
    left = col_ref[jnp.clip(my_c - 1, 0, cols - 2)]
    right = col_ref[jnp.clip(my_c, 0, cols - 2)]

    def offsets(d):
        dy, dx = STEPS[d]
        oy = up - PH if dy < 0 else PH - down if dy > 0 else 0
        ox = left - PW if dx < 0 else PW - right if dx > 0 else 0
        return oy, ox

    def slide(part, dy):
        count = STRIP // LANES
        base = (pixels - STRIP) if dy > 0 else 0
        oy = offsets(6 if dy > 0 else 1)[0]
        steps = (oy >> 1) - LOW if dy > 0 else 0 - LOW - (oy >> 1)
        stack = jnp.concatenate([wide[part, base + LANES * b:base + LANES * (b + 1)] for b in range(count)], axis=0)
        stack = jnp.concatenate([stack, stack[8 * (count - 1):]], axis=0)
        for bit in (3, 2, 1, 0):
            jump = 8 << bit
            chosen = jnp.broadcast_to(((steps >> bit) & 1) == 1, (8 * count + 8 - jump, LANES))
            if dy > 0:
                moved = jnp.where(chosen, stack[jump:], stack[:-jump])
                stack = jnp.concatenate([moved, stack[-jump:]], axis=0)
            else:
                moved = jnp.where(chosen, stack[:-jump], stack[jump:])
                stack = jnp.concatenate([stack[:jump], moved], axis=0)
        return stack

    def emit(d, first, masked, slid):
        oy, ox = offsets(d)
        dy, dx = STEPS[d]
        start, width = lanes_in(d, pixels)
        blocks = width // LANES
        part = slice(8 * (d // 2), 8 * (d // 2) + 8)
        low = PAD * (d % 2)
        if dy == 0:
            stack = jnp.concatenate([wide[part, LANES * b:LANES * (b + 1)] for b in range(blocks)], axis=0)
            stack = pltpu.roll(stack, (0 - ox) & (LANES - 1), 1)
        else:
            if (d // 2, dy) not in slid:
                slid[d // 2, dy] = slide(part, dy)
            odd = oy & 1
            stack = pltpu.roll(slid[d // 2, dy], (0 - ox - PW * odd) & (LANES - 1), 1)
            later = (iota((8 * blocks, LANES), 1) >= PW * (2 - odd))
            stack = jnp.where(later, stack[8:], stack[:-8])
        if masked:
            lane = iota((8 * blocks, LANES), 1)
            y = (start >> 6) + 2 * (iota((8 * blocks, LANES), 0) >> 3) + (lane >> 6) + oy
            x = (lane & (PW - 1)) + ox
            stack = jnp.where((y >= 0) & (y < PH) & (x >= 0) & (x < PW), stack, 0.0)
        for b in range(blocks):
            send[d, :, first + LANES * b:first + LANES * (b + 1)] = stack[8 * b + low:8 * b + low + PAD].astype(BF)

    fetches[3].wait()
    for first in range(0, pixels, CHUNK):
        wide[:, first:first + CHUNK] = dot(pick, foot_ref[0:nb, first:first + CHUNK])
    slid = {}
    for d in ORDER:
        emit(d, 0, True, slid)

    total = jnp.int32(0)
    for d in range(8):
        total = total + exists(d).astype(jnp.int32)
    pl.semaphore_wait(barrier, total)
    for d in ORDER:
        @pl.when(exists(d))
        def _():
            copy1(d).start()

    for fetch in fetches[4:]:
        fetch.wait()
    same = iota((slots, slots), 0) == iota((slots, slots), 1)

    def column(values):
        grid = jnp.where(same, values.astype(F32), 0.0)
        return jnp.sum(grid, axis=1, keepdims=True).astype(jnp.int32)

    ids = column(pair_ref[0])
    direction = column(pair_ref[1])
    place = column(pair_ref[2])
    live = iota((slots, 1), 0) < pair_count[0, 0]
    own_hot = ((iota((slots, comps), 1) == ids) & live).astype(BF)
    border_slot = PAD * direction + place
    border_hot = ((iota((slots, nbp), 1) == border_slot) & live).astype(BF)
    hit = lax.dot_general(border_hot, jnp.ones((slots, LANES), BF), (((0,), (0,)), ((), ())),
                          preferred_element_type=F32) > 0.5

    c_own = dot(own_hot, own_traces)
    c_own_bf = c_own.astype(BF)
    energy = jnp.sum(c_own * c_own, axis=1, keepdims=True)
    for first in range(0, pixels, CHUNK):
        span = slice(first, first + CHUNK)
        mine = dot(own_hot, foot_ref[:, span])
        a_own[:, span] = mine
        turned = jnp.transpose(res_ref[span, :])
        res_t[:, span] = turned
        shape[:, span] = dot(c_own_bf, turned) + mine * energy

    k = iota((nb, nbp), 0)
    k_dir = iota((nb, 1), 0)
    dir_of = jnp.zeros((nb, 1), jnp.int32)
    dir_wide = jnp.zeros((nb, nbp), jnp.int32)
    for d in range(1, 8):
        dir_of = dir_of + (k_dir >= NBR * d).astype(jnp.int32)
        dir_wide = dir_wide + (k >= NBR * d).astype(jnp.int32)
    squeeze = (iota((nb, nbp), 1) == PAD * dir_wide + k - NBR * dir_wide).astype(BF)
    alive = iota((comps, 1), 0) < comp_count[0, 0]
    alive_low = alive[0:nb]

    for d in RECEIVE:
        start, width = lanes_out(d, pixels)

        @pl.when(exists(d))
        def _():
            copy1(7 - d).wait_recv()
            border[PAD * d:PAD * d + PAD, start:start + width] = recv1[d, :, 0:width]
            border_trace[PAD * d:PAD * d + PAD, :] = recv1[d, :, width:width + frames]

    c_rem = dot(border_hot, border_trace[...])
    for first in range(0, pixels, CHUNK):
        span = slice(first, first + CHUNK)
        a_rem[:, span] = dot(border_hot, border[:, span])

    trace = c_own
    for t in range(ITERS):
        with_own = jnp.sum(c_own * trace, axis=1, keepdims=True)
        with_rem = jnp.sum(c_rem * trace, axis=1, keepdims=True)
        norm = 1.0 / (jnp.sum(trace * trace, axis=1, keepdims=True) + EPS * frames)
        trace_bf = trace.astype(BF)
        down_sum = jnp.zeros((slots, frames), F32)
        sum_own = jnp.zeros((slots, LANES), F32)
        sum_rem = jnp.zeros((slots, LANES), F32)
        sum_sq = jnp.zeros((slots, LANES), F32)
        for first in range(0, pixels, WIDE):
            span = slice(first, first + WIDE)
            mine = a_own[:, span]
            theirs = a_rem[:, span]
            if t == 0:
                across = shape[:, span]
            else:
                across = dot(trace_bf, res_t[:, span]) + mine * with_own
            foot = jnp.maximum(across + theirs * with_rem, 0.0) * norm
            sum_own = sum_own + narrow(mine * foot)
            sum_rem = sum_rem + narrow(theirs * foot)
            sum_sq = sum_sq + narrow(foot * foot)
            foot = foot.astype(BF)
            down_sum = down_sum + dot(foot, res_ref[span, :])
            if t == ITERS - 1:
                shape[:, span] = foot.astype(F32)
                wide[:, first:first + WIDE] = lax.dot_general(
                    border_hot, foot, (((0,), (0,)), ((), ())), preferred_element_type=F32)
        if t == ITERS - 1:
            slid = {}
            for d in ORDER:
                emit(d, span1(d), False, slid)
            for d in ORDER:
                @pl.when(exists(d))
                def _():
                    copy2(d).start()
        dot_own = jnp.sum(sum_own, axis=1, keepdims=True)
        dot_rem = jnp.sum(sum_rem, axis=1, keepdims=True)
        scale = 1.0 / (jnp.sum(sum_sq, axis=1, keepdims=True) + EPS * pixels)
        trace = jnp.maximum(down_sum + c_own * dot_own + c_rem * dot_rem, 0.0) * scale

    trace_bf = trace.astype(BF)
    sent = lax.dot_general(border_hot, trace_bf, (((0,), (0,)), ((), ())), preferred_element_type=F32)
    sent = jnp.where(hit, sent, -1.0)
    for d in range(8):
        first = span1(d) + lanes_in(d, pixels)[1]
        send[d, :, first:first + frames] = sent[PAD * d:PAD * d + PAD].astype(BF)
    for d in ORDER:
        @pl.when(exists(d))
        def _():
            copy3(d).start()

    upper = slice(nb, comps)
    hot_up = own_hot[:, upper]
    ones = jnp.ones((slots, 128), BF)
    hit_up = lax.dot_general(hot_up, ones, (((0,), (0,)), ((), ())), preferred_element_type=F32)[:, 0:1] > 0.5
    alive_up = alive[upper]
    for first in range(0, pixels, CHUNK):
        span = slice(first, first + CHUNK)
        new = lax.dot_general(hot_up, shape[:, span].astype(BF), (((0,), (0,)), ((), ())),
                              preferred_element_type=F32)
        new = jnp.where(hit_up, new, foot_ref[upper, span].astype(F32))
        out_foot[upper, span] = jnp.where(alive_up, new, 0.0).astype(BF)
    new = lax.dot_general(hot_up, trace_bf, (((0,), (0,)), ((), ())), preferred_element_type=F32)
    new = jnp.where(hit_up, new, own_traces[upper].astype(F32))
    out_trace[upper, :] = jnp.where(alive_up, new, 0.0).astype(BF)

    local = own_traces.astype(F32)
    local = local - jnp.mean(local, axis=1, keepdims=True)
    remote_traces = dot(squeeze, border_trace[...])
    remote_traces = remote_traces - jnp.mean(remote_traces, axis=1, keepdims=True)
    spread_remote = jnp.mean(remote_traces * remote_traces, axis=1, keepdims=True)
    full = functools.partial(lax.dot_general, dimension_numbers=(((1,), (1,)), ((), ())),
                             precision=lax.Precision.HIGHEST, preferred_element_type=F32)
    cov = full(remote_traces, local) / frames
    spread_local = full(jnp.ones((8, frames), F32), local * local)[0:1] / frames
    corr = cov / jnp.sqrt((spread_local + EPS) * (spread_remote + EPS))
    out_corr[...] = jnp.where(iota((1, comps), 1) < comp_count[0, 0], corr, 0.0)

    oy, ox = shift_of(dir_of, up, down, left, right)
    flat = dir_of + (dir_of >= 4).astype(jnp.int32)
    row = (flat >= 3).astype(jnp.int32) + (flat >= 6).astype(jnp.int32)
    dy = row - 1
    dx = flat - 3 * row - 1
    there = (my_r + dy >= 0) & (my_r + dy < rows) & (my_c + dx >= 0) & (my_c + dx < cols) & alive_low
    for first in range(0, pixels, CHUNK):
        span = slice(first, first + CHUNK)
        take[:, span] = jnp.where(inside_of(oy, ox, first, CHUNK) & there, 1.0, 0.0)
        keep[:, span] = jnp.where(alive_low, foot_ref[0:nb, span].astype(F32), 0.0)

    for d in RECEIVE:
        start, width = lanes_out(d, pixels)

        @pl.when(exists(d))
        def _():
            both(7 - d).wait_recv()
            back[PAD * d:PAD * d + PAD, start:start + width] = recv2[d, :, 0:width]
            back_trace[PAD * d:PAD * d + PAD, :] = recv2[d, :, width:width + frames]

    new = dot(squeeze, back_trace[...])
    came = new >= 0.0
    new = jnp.where(there & came, new, jnp.where(alive_low, own_traces[0:nb].astype(F32), 0.0))
    out_trace[0:nb, :] = new.astype(BF)
    came = jnp.where(came, 1.0, 0.0)
    came = jnp.concatenate([came] * (CHUNK // LANES), axis=1)
    for first in range(0, pixels, CHUNK):
        span = slice(first, first + CHUNK)
        new = dot(squeeze, back[:, span])
        out_foot[0:nb, span] = jnp.where(take[:, span] * came > 0.5, new, keep[:, span]).astype(BF)

    for d in range(8):
        @pl.when(exists(d))
        def _():
            all_sent(d).wait_send()


def store(foot, trace, corr, out_foot, out_trace, out_corr, sem):
    pairs = ((foot, out_foot), (trace, out_trace), (corr, out_corr))
    copies = [pltpu.make_async_copy(a, b, sem.at[i]) for i, (a, b) in enumerate(pairs)]
    for copy in copies:
        copy.start()
    for copy in copies:
        copy.wait()


def shards(rows, cols, residual, footprints, traces, merge_pairs, pair_counts, comp_counts, row_int, col_int):
    pixels, frames = residual.shape[2:]
    comps = footprints.shape[2]
    slots = merge_pairs.shape[2]
    nb, nbp = 8 * NBR, 8 * PAD
    vmem = pl.BlockSpec(memory_space=pltpu.VMEM)
    smem = pl.BlockSpec(memory_space=pltpu.SMEM)
    hbm = pl.BlockSpec(memory_space=pltpu.HBM)
    i32 = jnp.int32
    both = pltpu.VMEM((8, PAD, pixels + frames), BF)
    pairs = jnp.transpose(merge_pairs, (0, 3, 1, 2))[0]
    out_shape = (
        jax.ShapeDtypeStruct((comps, pixels), BF),
        jax.ShapeDtypeStruct((comps, frames), BF),
        jax.ShapeDtypeStruct((nb, comps), F32),
    )
    results = pl.pallas_call(
        functools.partial(kernel, rows, cols),
        out_shape=out_shape,
        in_specs=[hbm] * 4 + [smem] * 2 + [hbm] * 2,
        out_specs=(vmem,) * 3,
        scratch_shapes=[
            pltpu.VMEM((pixels, frames), BF), pltpu.VMEM((comps, pixels), BF), pltpu.VMEM((comps, frames), BF),
            pltpu.VMEM((3, 1, slots), i32),
            pltpu.SMEM(row_int.shape, i32), pltpu.SMEM(col_int.shape, i32), pltpu.SemaphoreType.DMA((7,)),
            pltpu.VMEM((8, PAD, 2 * (pixels + frames)), BF), both, both,
            pltpu.VMEM((nbp, pixels), F32), pltpu.VMEM((frames, pixels), BF),
            pltpu.VMEM((nbp, pixels), BF), pltpu.VMEM((nbp, frames), BF),
            pltpu.VMEM((nbp, pixels), BF), pltpu.VMEM((nbp, frames), BF),
            pltpu.VMEM((slots, pixels), F32), pltpu.VMEM((slots, pixels), F32),
            pltpu.VMEM((slots, pixels), F32),
            pltpu.VMEM((nb, pixels), F32), pltpu.VMEM((nb, pixels), F32),
            pltpu.SemaphoreType.DMA((8,)), pltpu.SemaphoreType.DMA((2, 8)),
        ],
        compiler_params=pltpu.CompilerParams(
            collective_id=0, has_side_effects=True, vmem_limit_bytes=32 * 1024 * 1024),
    )(*[pltpu.with_memory_space_constraint(x, pltpu.HBM) for x in (
        residual[0, 0], footprints[0, 0], traces[0, 0], pairs)], pair_counts, comp_counts,
      *[pltpu.with_memory_space_constraint(x, pltpu.HBM) for x in (row_int, col_int)])
    foot, trace, corr = pl.pallas_call(
        store,
        out_shape=out_shape,
        in_specs=[vmem] * 3,
        out_specs=(hbm,) * 3,
        scratch_shapes=[pltpu.SemaphoreType.DMA((3,))],
        compiler_params=pltpu.CompilerParams(vmem_limit_bytes=4 * 1024 * 1024),
    )(*results)
    return foot[None, None], trace[None, None], jnp.transpose(corr)[None, None]


def solution(mesh):
    rows, cols = mesh.shape["py"], mesh.shape["px"]
    spec = P("py", "px", None, None)
    return jax.shard_map(
        functools.partial(shards, rows, cols), mesh=mesh,
        in_specs=(spec, spec, spec, spec, P("py", "px"), P("py", "px"), P(), P()),
        out_specs=(spec, spec, spec), check_vma=False)
```

```python
import functools

import jax
import jax.numpy as jnp
from jax import lax
from jax.experimental import pallas as pl
from jax.experimental.pallas import tpu as pltpu
from jax.sharding import PartitionSpec as P

PH = 64
PW = 64
NBR = 3
OV_HI = 24
ITERS = 4
EPS = 1e-05

PAD = 4
STRIP = OV_HI * PW
CHUNK = 512
WIDE = 1024
LANES = 128
LOW = (PH - OV_HI) // 2
ORDER = (0, 2, 5, 7, 1, 6, 3, 4)
RECEIVE = (3, 4, 1, 6, 0, 2, 5, 7)
STEPS = [(-1, -1), (-1, 0), (-1, 1), (0, -1), (0, 1), (1, -1), (1, 0), (1, 1)]
BF = jnp.bfloat16
F32 = jnp.float32
MESH = pl.DeviceIdType.MESH


def lanes_in(direction, pixels):
    dy = STEPS[direction][0]
    if dy > 0:
        return (0, STRIP)
    if dy < 0:
        return (pixels - STRIP, STRIP)
    return (0, pixels)


def lanes_out(direction, pixels):
    return lanes_in(7 - direction, pixels)


def dot(a, b):
    return jnp.dot(a, b, preferred_element_type=F32)


def dot_t(a, b):
    return lax.dot_general(a, b, (((1,), (1,)), ((), ())), preferred_element_type=F32)


def iota(shape, dim):
    return lax.broadcasted_iota(jnp.int32, shape, dim)


def narrow(x):
    return functools.reduce(jnp.add, [x[:, b:b + LANES] for b in range(0, x.shape[1], LANES)])


def shift_of(direction, up, down, left, right):
    flat = direction + (direction >= 4).astype(jnp.int32)
    row = (flat >= 3).astype(jnp.int32) + (flat >= 6).astype(jnp.int32)
    dy = row - 1
    dx = flat - 3 * row - 1
    oy = jnp.where(dy < 0, up - PH, jnp.where(dy > 0, PH - down, 0))
    ox = jnp.where(dx < 0, left - PW, jnp.where(dx > 0, PW - right, 0))
    return oy, ox


def inside_of(oy, ox, first, count):
    pixel = iota((1, count), 1) + first
    y = (pixel >> 6) - oy
    x = (pixel & (PW - 1)) - ox
    return (y >= 0) & (y < PH) & (x >= 0) & (x < PW)


def kernel(
    rows, cols,
    res_hbm, foot_hbm, trace_hbm, pair_hbm, pair_count, comp_count, row_hbm, col_hbm,
    out_foot, out_trace, out_corr,
    res_ref, foot_ref, trace_ref, pair_ref, row_ref, col_ref, sem_in,
    send, recv1, recv2, wide, res_t,
    border, border_trace, back, back_trace, a_own, a_rem, shape, feet, take, keep,
    sem_s, sem_r,
):
    pixels = foot_ref.shape[1]
    frames = trace_ref.shape[1]
    comps = foot_ref.shape[0]
    slots = pair_ref.shape[2]
    nb = 8 * NBR
    nbp = 8 * PAD
    my_r = lax.axis_index("py")
    my_c = lax.axis_index("px")

    def target(d):
        return (my_r + STEPS[d][0], my_c + STEPS[d][1])

    def exists(d):
        r, c = target(d)
        return (r >= 0) & (r < rows) & (c >= 0) & (c < cols)

    barrier = pltpu.get_barrier_semaphore()
    for d in range(8):
        @pl.when(exists(d))
        def _():
            pl.semaphore_signal(barrier, 1, device_id=target(d), device_id_type=MESH)
    fetches = [
        (trace_hbm, trace_ref),
        (row_hbm, row_ref), (col_hbm, col_ref),
        (foot_hbm.at[pl.ds(0, nb)], foot_ref.at[pl.ds(0, nb)]),
        (pair_hbm, pair_ref),
        (foot_hbm.at[pl.ds(nb, comps - nb)], foot_ref.at[pl.ds(nb, comps - nb)]),
        (res_hbm, res_ref),
    ]
    fetches = [pltpu.make_async_copy(a, b, sem_in.at[i]) for i, (a, b) in enumerate(fetches)]
    for fetch in fetches:
        fetch.start()

    def span1(d):
        return lanes_in(d, pixels)[1] + frames

    def remote(src, dst, d, phase):
        return pltpu.make_async_remote_copy(
            src, dst, sem_s.at[d], sem_r.at[phase, 7 - d],
            device_id=target(d), device_id_type=MESH)

    def copy1(d):
        part = pl.ds(0, span1(d))
        return remote(send.at[d, :, part], recv1.at[7 - d, :, part], d, 0)

    def both(d):
        part = pl.ds(0, span1(d))
        return remote(send.at[d, :, pl.ds(span1(d), span1(d))], recv2.at[7 - d, :, part], d, 1)

    def all_sent(d):
        part = send.at[d, :, pl.ds(0, 2 * span1(d))]
        return remote(part, part, d, 1)

    j = iota((nbp, nb), 0)
    pick = (((j & (PAD - 1)) < NBR) & (iota((nbp, nb), 1) == NBR * (j >> 2) + (j & (PAD - 1)))).astype(BF)
    border[...] = jnp.zeros_like(border)
    border_trace[...] = jnp.zeros_like(border_trace)
    back[...] = jnp.zeros_like(back)
    back_trace[...] = jnp.zeros_like(back_trace)
    fetches[0].wait()
    own_traces = trace_ref[...]
    packed_traces = dot(pick, own_traces[0:nb])
    for d in range(8):
        width = lanes_in(d, pixels)[1]
        send[d, :, width:width + frames] = packed_traces[PAD * d:PAD * d + PAD].astype(BF)
    fetches[1].wait()
    fetches[2].wait()
    up = row_ref[jnp.clip(my_r - 1, 0, rows - 2)]
    down = row_ref[jnp.clip(my_r, 0, rows - 2)]
    left = col_ref[jnp.clip(my_c - 1, 0, cols - 2)]
    right = col_ref[jnp.clip(my_c, 0, cols - 2)]

    def offsets(d):
        dy, dx = STEPS[d]
        oy = up - PH if dy < 0 else PH - down if dy > 0 else 0
        ox = left - PW if dx < 0 else PW - right if dx > 0 else 0
        return oy, ox

    def slide(part, dy):
        count = STRIP // LANES
        base = (pixels - STRIP) if dy > 0 else 0
        oy = offsets(6 if dy > 0 else 1)[0]
        steps = (oy >> 1) - LOW if dy > 0 else 0 - LOW - (oy >> 1)
        stack = jnp.concatenate([wide[part, base + LANES * b:base + LANES * (b + 1)] for b in range(count)], axis=0)
        stack = jnp.concatenate([stack, stack[8 * (count - 1):]], axis=0)
        for bit in (3, 2, 1, 0):
            jump = 8 << bit
            chosen = jnp.broadcast_to(((steps >> bit) & 1) == 1, (8 * count + 8 - jump, LANES))
            if dy > 0:
                moved = jnp.where(chosen, stack[jump:], stack[:-jump])
                stack = jnp.concatenate([moved, stack[-jump:]], axis=0)
            else:
                moved = jnp.where(chosen, stack[:-jump], stack[jump:])
                stack = jnp.concatenate([stack[:jump], moved], axis=0)
        return stack

    def emit(d, first, masked, slid):
        oy, ox = offsets(d)
        dy, dx = STEPS[d]
        start, width = lanes_in(d, pixels)
        blocks = width // LANES
        part = slice(8 * (d // 2), 8 * (d // 2) + 8)
        low = PAD * (d % 2)
        if dy == 0:
            stack = jnp.concatenate([wide[part, LANES * b:LANES * (b + 1)] for b in range(blocks)], axis=0)
            stack = pltpu.roll(stack, (0 - ox) & (LANES - 1), 1)
        else:
            if (d // 2, dy) not in slid:
                slid[d // 2, dy] = slide(part, dy)
            odd = oy & 1
            stack = pltpu.roll(slid[d // 2, dy], (0 - ox - PW * odd) & (LANES - 1), 1)
            later = (iota((8 * blocks, LANES), 1) >= PW * (2 - odd))
            stack = jnp.where(later, stack[8:], stack[:-8])
        if masked:
            lane = iota((8 * blocks, LANES), 1)
            y = (start >> 6) + 2 * (iota((8 * blocks, LANES), 0) >> 3) + (lane >> 6) + oy
            x = (lane & (PW - 1)) + ox
            stack = jnp.where((y >= 0) & (y < PH) & (x >= 0) & (x < PW), stack, 0.0)
        for b in range(blocks):
            send[d, :, first + LANES * b:first + LANES * (b + 1)] = stack[8 * b + low:8 * b + low + PAD].astype(BF)

    fetches[3].wait()
    for first in range(0, pixels, CHUNK):
        wide[:, first:first + CHUNK] = dot(pick, foot_ref[0:nb, first:first + CHUNK])
    slid = {}
    for d in ORDER:
        emit(d, 0, True, slid)

    total = jnp.int32(0)
    for d in range(8):
        total = total + exists(d).astype(jnp.int32)
    pl.semaphore_wait(barrier, total)
    for d in ORDER:
        @pl.when(exists(d))
        def _():
            copy1(d).start()

    for fetch in fetches[4:]:
        fetch.wait()
    same = iota((slots, slots), 0) == iota((slots, slots), 1)

    def column(values):
        grid = jnp.where(same, values.astype(F32), 0.0)
        return jnp.sum(grid, axis=1, keepdims=True).astype(jnp.int32)

    ids = column(pair_ref[0])
    direction = column(pair_ref[1])
    place = column(pair_ref[2])
    live = iota((slots, 1), 0) < pair_count[0, 0]
    own_hot = ((iota((slots, comps), 1) == ids) & live).astype(BF)
    border_slot = PAD * direction + place
    border_hot = ((iota((slots, nbp), 1) == border_slot) & live).astype(BF)
    hit = lax.dot_general(border_hot, jnp.ones((slots, LANES), BF), (((0,), (0,)), ((), ())),
                          preferred_element_type=F32) > 0.5

    c_own = dot(own_hot, own_traces)
    c_own_bf = c_own.astype(BF)
    energy = jnp.sum(c_own * c_own, axis=1, keepdims=True)
    for first in range(0, pixels, CHUNK):
        span = slice(first, first + CHUNK)
        mine = dot(own_hot, foot_ref[:, span])
        a_own[:, span] = mine
        turned = jnp.transpose(res_ref[span, :])
        res_t[:, span] = turned
        shape[:, span] = dot(c_own_bf, turned) + mine * energy

    k = iota((nb, nbp), 0)
    k_dir = iota((nb, 1), 0)
    dir_of = jnp.zeros((nb, 1), jnp.int32)
    dir_wide = jnp.zeros((nb, nbp), jnp.int32)
    for d in range(1, 8):
        dir_of = dir_of + (k_dir >= NBR * d).astype(jnp.int32)
        dir_wide = dir_wide + (k >= NBR * d).astype(jnp.int32)
    squeeze = (iota((nb, nbp), 1) == PAD * dir_wide + k - NBR * dir_wide).astype(BF)
    alive = iota((comps, 1), 0) < comp_count[0, 0]
    alive_low = alive[0:nb]

    for d in RECEIVE:
        start, width = lanes_out(d, pixels)

        @pl.when(exists(d))
        def _():
            copy1(7 - d).wait_recv()
            border[PAD * d:PAD * d + PAD, start:start + width] = recv1[d, :, 0:width]
            border_trace[PAD * d:PAD * d + PAD, :] = recv1[d, :, width:width + frames]

    c_rem = dot(border_hot, border_trace[...])
    a_rem[...] = dot(border_hot, border[...])

    trace = c_own
    for t in range(ITERS):
        with_own = jnp.sum(c_own * trace, axis=1, keepdims=True)
        with_rem = jnp.sum(c_rem * trace, axis=1, keepdims=True)
        norm = 1.0 / (jnp.sum(trace * trace, axis=1, keepdims=True) + EPS * frames)
        trace_bf = trace.astype(BF)
        sum_own = jnp.zeros((slots, LANES), F32)
        sum_rem = jnp.zeros((slots, LANES), F32)
        sum_sq = jnp.zeros((slots, LANES), F32)
        for first in range(0, pixels, WIDE):
            span = slice(first, first + WIDE)
            mine = a_own[:, span]
            theirs = a_rem[:, span]
            if t == 0:
                across = shape[:, span]
            else:
                across = dot(trace_bf, res_t[:, span]) + mine * with_own
            foot = jnp.maximum(across + theirs * with_rem, 0.0) * norm
            sum_own = sum_own + narrow(mine * foot)
            sum_rem = sum_rem + narrow(theirs * foot)
            sum_sq = sum_sq + narrow(foot * foot)
            feet[:, span] = foot.astype(BF)
        if t == ITERS - 1:
            for first in range(0, pixels, WIDE):
                wide[:, first:first + WIDE] = lax.dot_general(
                    border_hot, feet[:, first:first + WIDE], (((0,), (0,)), ((), ())), preferred_element_type=F32)
        down_sum = dot(feet[...], res_ref[...])
        if t == ITERS - 1:
            slid = {}
            for d in ORDER:
                emit(d, span1(d), False, slid)
        dot_own = jnp.sum(sum_own, axis=1, keepdims=True)
        dot_rem = jnp.sum(sum_rem, axis=1, keepdims=True)
        scale = 1.0 / (jnp.sum(sum_sq, axis=1, keepdims=True) + EPS * pixels)
        trace = jnp.maximum(down_sum + c_own * dot_own + c_rem * dot_rem, 0.0) * scale

    trace_bf = trace.astype(BF)
    sent = lax.dot_general(border_hot, trace_bf, (((0,), (0,)), ((), ())), preferred_element_type=F32)
    sent = jnp.where(hit, sent, -1.0)
    for d in range(8):
        first = span1(d) + lanes_in(d, pixels)[1]
        send[d, :, first:first + frames] = sent[PAD * d:PAD * d + PAD].astype(BF)
    for d in ORDER:
        @pl.when(exists(d))
        def _():
            both(d).start()

    upper = slice(nb, comps)
    hot_up = own_hot[:, upper]
    ones = jnp.ones((slots, 128), BF)
    hit_up = lax.dot_general(hot_up, ones, (((0,), (0,)), ((), ())), preferred_element_type=F32)[:, 0:1] > 0.5
    alive_up = alive[upper]
    for first in range(0, pixels, CHUNK):
        span = slice(first, first + CHUNK)
        new = lax.dot_general(hot_up, feet[:, span], (((0,), (0,)), ((), ())), preferred_element_type=F32)
        new = jnp.where(hit_up, new, foot_ref[upper, span].astype(F32))
        out_foot[upper, span] = jnp.where(alive_up, new, 0.0).astype(BF)
    new = lax.dot_general(hot_up, trace_bf, (((0,), (0,)), ((), ())), preferred_element_type=F32)
    new = jnp.where(hit_up, new, own_traces[upper].astype(F32))
    out_trace[upper, :] = jnp.where(alive_up, new, 0.0).astype(BF)

    local = own_traces.astype(F32)
    local = local - jnp.mean(local, axis=1, keepdims=True)
    remote_traces = dot(squeeze, border_trace[...])
    remote_traces = remote_traces - jnp.mean(remote_traces, axis=1, keepdims=True)
    spread_remote = jnp.mean(remote_traces * remote_traces, axis=1, keepdims=True)
    full = functools.partial(lax.dot_general, dimension_numbers=(((1,), (1,)), ((), ())),
                             precision=lax.Precision.HIGHEST, preferred_element_type=F32)
    cov = full(remote_traces, local) / frames
    spread_local = full(jnp.ones((8, frames), F32), local * local)[0:1] / frames
    corr = cov / jnp.sqrt((spread_local + EPS) * (spread_remote + EPS))
    out_corr[...] = jnp.where(iota((1, comps), 1) < comp_count[0, 0], corr, 0.0)

    oy, ox = shift_of(dir_of, up, down, left, right)
    flat = dir_of + (dir_of >= 4).astype(jnp.int32)
    row = (flat >= 3).astype(jnp.int32) + (flat >= 6).astype(jnp.int32)
    dy = row - 1
    dx = flat - 3 * row - 1
    there = (my_r + dy >= 0) & (my_r + dy < rows) & (my_c + dx >= 0) & (my_c + dx < cols) & alive_low
    for first in range(0, pixels, CHUNK):
        span = slice(first, first + CHUNK)
        take[:, span] = jnp.where(inside_of(oy, ox, first, CHUNK) & there, 1.0, 0.0)
        keep[:, span] = jnp.where(alive_low, foot_ref[0:nb, span].astype(F32), 0.0)

    for d in RECEIVE:
        start, width = lanes_out(d, pixels)

        @pl.when(exists(d))
        def _():
            both(7 - d).wait_recv()
            back[PAD * d:PAD * d + PAD, start:start + width] = recv2[d, :, 0:width]
            back_trace[PAD * d:PAD * d + PAD, :] = recv2[d, :, width:width + frames]

    new = dot(squeeze, back_trace[...])
    came = new >= 0.0
    new = jnp.where(there & came, new, jnp.where(alive_low, own_traces[0:nb].astype(F32), 0.0))
    out_trace[0:nb, :] = new.astype(BF)
    came = jnp.where(came, 1.0, 0.0)
    came = jnp.concatenate([came] * (CHUNK // LANES), axis=1)
    wide[0:nb, :] = dot(squeeze, back[...])
    for first in range(0, pixels, CHUNK):
        span = slice(first, first + CHUNK)
        new = wide[0:nb, span]
        out_foot[0:nb, span] = jnp.where(take[:, span] * came > 0.5, new, keep[:, span]).astype(BF)

    for d in range(8):
        @pl.when(exists(d))
        def _():
            all_sent(d).wait_send()


def store(foot, trace, corr, out_foot, out_trace, out_corr, sem):
    pairs = ((foot, out_foot), (trace, out_trace), (corr, out_corr))
    copies = [pltpu.make_async_copy(a, b, sem.at[i]) for i, (a, b) in enumerate(pairs)]
    for copy in copies:
        copy.start()
    for copy in copies:
        copy.wait()


def shards(rows, cols, residual, footprints, traces, merge_pairs, pair_counts, comp_counts, row_int, col_int):
    pixels, frames = residual.shape[2:]
    comps = footprints.shape[2]
    slots = merge_pairs.shape[2]
    nb, nbp = 8 * NBR, 8 * PAD
    vmem = pl.BlockSpec(memory_space=pltpu.VMEM)
    smem = pl.BlockSpec(memory_space=pltpu.SMEM)
    hbm = pl.BlockSpec(memory_space=pltpu.HBM)
    i32 = jnp.int32
    both = pltpu.VMEM((8, PAD, pixels + frames), BF)
    pairs = jnp.transpose(merge_pairs, (0, 3, 1, 2))[0]
    out_shape = (
        jax.ShapeDtypeStruct((comps, pixels), BF),
        jax.ShapeDtypeStruct((comps, frames), BF),
        jax.ShapeDtypeStruct((nb, comps), F32),
    )
    results = pl.pallas_call(
        functools.partial(kernel, rows, cols),
        out_shape=out_shape,
        in_specs=[hbm] * 4 + [smem] * 2 + [hbm] * 2,
        out_specs=(vmem,) * 3,
        scratch_shapes=[
            pltpu.VMEM((pixels, frames), BF), pltpu.VMEM((comps, pixels), BF), pltpu.VMEM((comps, frames), BF),
            pltpu.VMEM((3, 1, slots), i32),
            pltpu.SMEM(row_int.shape, i32), pltpu.SMEM(col_int.shape, i32), pltpu.SemaphoreType.DMA((7,)),
            pltpu.VMEM((8, PAD, 2 * (pixels + frames)), BF), both, both,
            pltpu.VMEM((nbp, pixels), F32), pltpu.VMEM((frames, pixels), BF),
            pltpu.VMEM((nbp, pixels), BF), pltpu.VMEM((nbp, frames), BF),
            pltpu.VMEM((nbp, pixels), BF), pltpu.VMEM((nbp, frames), BF),
            pltpu.VMEM((slots, pixels), F32), pltpu.VMEM((slots, pixels), F32),
            pltpu.VMEM((slots, pixels), F32), pltpu.VMEM((slots, pixels), BF),
            pltpu.VMEM((nb, pixels), F32), pltpu.VMEM((nb, pixels), F32),
            pltpu.SemaphoreType.DMA((8,)), pltpu.SemaphoreType.DMA((2, 8)),
        ],
        compiler_params=pltpu.CompilerParams(
            collective_id=0, has_side_effects=True, vmem_limit_bytes=32 * 1024 * 1024),
    )(*[pltpu.with_memory_space_constraint(x, pltpu.HBM) for x in (
        residual[0, 0], footprints[0, 0], traces[0, 0], pairs)], pair_counts, comp_counts,
      *[pltpu.with_memory_space_constraint(x, pltpu.HBM) for x in (row_int, col_int)])
    foot, trace, corr = pl.pallas_call(
        store,
        out_shape=out_shape,
        in_specs=[vmem] * 3,
        out_specs=(hbm,) * 3,
        scratch_shapes=[pltpu.SemaphoreType.DMA((3,))],
        compiler_params=pltpu.CompilerParams(vmem_limit_bytes=4 * 1024 * 1024),
    )(*results)
    return foot[None, None], trace[None, None], jnp.transpose(corr)[None, None]


def solution(mesh):
    rows, cols = mesh.shape["py"], mesh.shape["px"]
    spec = P("py", "px", None, None)
    return jax.shard_map(
        functools.partial(shards, rows, cols), mesh=mesh,
        in_specs=(spec, spec, spec, spec, P("py", "px"), P("py", "px"), P(), P()),
        out_specs=(spec, spec, spec), check_vma=False)
```

```python
import functools

import jax
import jax.numpy as jnp
from jax import lax
from jax.experimental import pallas as pl
from jax.experimental.pallas import tpu as pltpu
from jax.sharding import PartitionSpec as P

PH = 64
PW = 64
NBR = 3
OV_HI = 24
ITERS = 4
EPS = 1e-05

PAD = 4
STRIP = OV_HI * PW
CHUNK = 512
WIDE = 1024
LANES = 128
LOW = (PH - OV_HI) // 2
ORDER = (0, 2, 5, 7, 1, 6, 3, 4)
RECEIVE = (3, 4, 1, 6, 0, 2, 5, 7)
STEPS = [(-1, -1), (-1, 0), (-1, 1), (0, -1), (0, 1), (1, -1), (1, 0), (1, 1)]
BF = jnp.bfloat16
F32 = jnp.float32
MESH = pl.DeviceIdType.MESH


def lanes_in(direction, pixels):
    dy = STEPS[direction][0]
    if dy > 0:
        return (0, STRIP)
    if dy < 0:
        return (pixels - STRIP, STRIP)
    return (0, pixels)


def lanes_out(direction, pixels):
    return lanes_in(7 - direction, pixels)


def dot(a, b):
    return jnp.dot(a, b, preferred_element_type=F32)


def dot_t(a, b):
    return lax.dot_general(a, b, (((1,), (1,)), ((), ())), preferred_element_type=F32)


def iota(shape, dim):
    return lax.broadcasted_iota(jnp.int32, shape, dim)


def narrow(x):
    return functools.reduce(jnp.add, [x[:, b:b + LANES] for b in range(0, x.shape[1], LANES)])


def inside_of(oy, ox, first, count):
    pixel = iota((1, count), 1) + first
    y = (pixel >> 6) - oy
    x = (pixel & (PW - 1)) - ox
    return (y >= 0) & (y < PH) & (x >= 0) & (x < PW)


def kernel(
    rows, cols,
    res_hbm, foot_hbm, trace_hbm, pair_hbm, pair_count, comp_count, row_hbm, col_hbm,
    out_foot, out_trace, out_corr,
    res_ref, foot_ref, trace_ref, pair_ref, row_ref, col_ref,
    send, recv1, recv2, wide, res_t,
    border, border_trace, a_own, a_rem, shape, feet, final, final_trace,
    sem_s, sem_r,
):
    pixels = foot_ref.shape[1]
    frames = trace_ref.shape[1]
    comps = foot_ref.shape[0]
    slots = pair_ref.shape[2]
    nb = 8 * NBR
    nbp = 8 * PAD
    my_r = lax.axis_index("py")
    my_c = lax.axis_index("px")

    def target(d):
        return (my_r + STEPS[d][0], my_c + STEPS[d][1])

    def exists(d):
        r, c = target(d)
        return (r >= 0) & (r < rows) & (c >= 0) & (c < cols)

    barrier = pltpu.get_barrier_semaphore()
    for d in ORDER:
        @pl.when(exists(d))
        def _():
            pl.semaphore_signal(barrier, 1, device_id=target(d), device_id_type=MESH)
    fetches = [
        (trace_hbm, trace_ref),
        (row_hbm, row_ref), (col_hbm, col_ref),
        (foot_hbm.at[pl.ds(0, nb)], foot_ref.at[pl.ds(0, nb)]),
        (pair_hbm, pair_ref),
        (foot_hbm.at[pl.ds(nb, comps - nb)], foot_ref.at[pl.ds(nb, comps - nb)]),
        (res_hbm, res_ref),
    ]
    fetches = [pltpu.make_async_copy(a, b, sem_s.at[i]) for i, (a, b) in enumerate(fetches)]
    for fetch in fetches:
        fetch.start()

    def span1(d):
        return lanes_in(d, pixels)[1] + frames

    def remote(src, dst, d, phase):
        return pltpu.make_async_remote_copy(
            src, dst, sem_s.at[d], sem_r.at[phase, 7 - d],
            device_id=target(d), device_id_type=MESH)

    def copy1(d):
        part = pl.ds(0, span1(d))
        return remote(send.at[d, :, part], recv1.at[7 - d, :, part], d, 0)

    def both(d):
        part = pl.ds(0, span1(d))
        return remote(send.at[d, :, pl.ds(span1(d), span1(d))], recv2.at[7 - d, :, part], d, 1)

    def issue(copy):
        odd = (my_c & 1) == 1
        for d, when in ((2, odd), (7, odd), (0, None), (5, None), (2, ~odd), (7, ~odd), (1, None), (6, None), (3, None), (4, None)):
            @pl.when(exists(d) if when is None else exists(d) & when)
            def _():
                copy(d).start()

    def all_sent(d):
        part = send.at[d, :, pl.ds(0, 2 * span1(d))]
        return remote(part, part, d, 1)

    j = iota((nbp, nb), 0)
    pick = (((j & (PAD - 1)) < NBR) & (iota((nbp, nb), 1) == NBR * (j >> 2) + (j & (PAD - 1)))).astype(BF)
    border[...] = jnp.zeros_like(border)
    border_trace[...] = jnp.zeros_like(border_trace)
    fetches[0].wait()
    own_traces = trace_ref[...]
    packed_traces = dot(pick, own_traces[0:nb])
    for d in range(8):
        width = lanes_in(d, pixels)[1]
        send[d, :, width:width + frames] = packed_traces[PAD * d:PAD * d + PAD].astype(BF)
    fetches[1].wait()
    fetches[2].wait()
    up = row_ref[jnp.clip(my_r - 1, 0, rows - 2)]
    down = row_ref[jnp.clip(my_r, 0, rows - 2)]
    left = col_ref[jnp.clip(my_c - 1, 0, cols - 2)]
    right = col_ref[jnp.clip(my_c, 0, cols - 2)]

    def offsets(d):
        dy, dx = STEPS[d]
        oy = up - PH if dy < 0 else PH - down if dy > 0 else 0
        ox = left - PW if dx < 0 else PW - right if dx > 0 else 0
        return oy, ox

    def slide(part, dy):
        count = STRIP // LANES
        base = (pixels - STRIP) if dy > 0 else 0
        oy = offsets(6 if dy > 0 else 1)[0]
        steps = (oy >> 1) - LOW if dy > 0 else 0 - LOW - (oy >> 1)
        stack = jnp.concatenate([wide[part, base + LANES * b:base + LANES * (b + 1)] for b in range(count)], axis=0)
        stack = jnp.concatenate([stack, stack[8 * (count - 1):]], axis=0)
        for bit in (3, 2, 1, 0):
            jump = 8 << bit
            chosen = jnp.broadcast_to(((steps >> bit) & 1) == 1, (8 * count + 8 - jump, LANES))
            if dy > 0:
                moved = jnp.where(chosen, stack[jump:], stack[:-jump])
                stack = jnp.concatenate([moved, stack[-jump:]], axis=0)
            else:
                moved = jnp.where(chosen, stack[:-jump], stack[jump:])
                stack = jnp.concatenate([stack[:jump], moved], axis=0)
        return stack

    def emit(d, first, masked, slid):
        oy, ox = offsets(d)
        dy, dx = STEPS[d]
        start, width = lanes_in(d, pixels)
        blocks = width // LANES
        part = slice(8 * (d // 2), 8 * (d // 2) + 8)
        low = PAD * (d % 2)
        if dy == 0:
            stack = jnp.concatenate([wide[part, LANES * b:LANES * (b + 1)] for b in range(blocks)], axis=0)
            stack = pltpu.roll(stack, (0 - ox) & (LANES - 1), 1)
        else:
            if (d // 2, dy) not in slid:
                slid[d // 2, dy] = slide(part, dy)
            odd = oy & 1
            stack = pltpu.roll(slid[d // 2, dy], (0 - ox - PW * odd) & (LANES - 1), 1)
            later = (iota((8 * blocks, LANES), 1) >= PW * (2 - odd))
            stack = jnp.where(later, stack[8:], stack[:-8])
        if masked:
            lane = iota((8 * blocks, LANES), 1)
            y = (start >> 6) + 2 * (iota((8 * blocks, LANES), 0) >> 3) + (lane >> 6) + oy
            x = (lane & (PW - 1)) + ox
            stack = jnp.where((y >= 0) & (y < PH) & (x >= 0) & (x < PW), stack, 0.0)
        for b in range(blocks):
            send[d, :, first + LANES * b:first + LANES * (b + 1)] = stack[8 * b + low:8 * b + low + PAD].astype(BF)

    fetches[3].wait()
    for first in range(0, pixels, CHUNK):
        wide[:, first:first + CHUNK] = dot(pick, foot_ref[0:nb, first:first + CHUNK])
    slid = {}
    for d in ORDER:
        emit(d, 0, True, slid)

    for fetch in fetches[4:]:
        fetch.wait()
    total = jnp.int32(0)
    for d in range(8):
        total = total + exists(d).astype(jnp.int32)
    pl.semaphore_wait(barrier, total)
    issue(copy1)

    same = iota((slots, slots), 0) == iota((slots, slots), 1)

    def column(values):
        grid = jnp.where(same, values.astype(F32), 0.0)
        return jnp.sum(grid, axis=1, keepdims=True).astype(jnp.int32)

    ids = column(pair_ref[0])
    direction = column(pair_ref[1])
    place = column(pair_ref[2])
    live = iota((slots, 1), 0) < pair_count[0, 0]
    own_hot = ((iota((slots, comps), 1) == ids) & live).astype(BF)
    border_slot = PAD * direction + place
    border_hot = ((iota((slots, nbp), 1) == border_slot) & live).astype(BF)
    hit = lax.dot_general(border_hot, jnp.ones((slots, LANES), BF), (((0,), (0,)), ((), ())),
                          preferred_element_type=F32) > 0.5

    c_own = dot(own_hot, own_traces)
    c_own_bf = c_own.astype(BF)
    energy = jnp.sum(c_own * c_own, axis=1, keepdims=True)
    for first in range(0, pixels, CHUNK):
        span = slice(first, first + CHUNK)
        mine = dot(own_hot, foot_ref[:, span])
        a_own[:, span] = mine
        turned = jnp.transpose(res_ref[span, :])
        res_t[:, span] = turned
        shape[:, span] = dot(c_own_bf, turned) + mine * energy

    k = iota((nb, nbp), 0)
    dir_wide = jnp.zeros((nb, nbp), jnp.int32)
    for d in range(1, 8):
        dir_wide = dir_wide + (k >= NBR * d).astype(jnp.int32)
    squeeze = (iota((nb, nbp), 1) == PAD * dir_wide + k - NBR * dir_wide).astype(BF)
    alive = iota((comps, 1), 0) < comp_count[0, 0]
    alive_low = alive[0:nb]

    for d in RECEIVE:
        start, width = lanes_out(d, pixels)

        @pl.when(exists(d))
        def _():
            copy1(7 - d).wait_recv()
            border[PAD * d:PAD * d + PAD, start:start + width] = recv1[d, :, 0:width]
            border_trace[PAD * d:PAD * d + PAD, :] = recv1[d, :, width:width + frames]

    c_rem = dot(border_hot, border_trace[...])
    a_rem[...] = dot(border_hot, border[...])

    trace = c_own
    for t in range(ITERS):
        with_own = jnp.sum(c_own * trace, axis=1, keepdims=True)
        with_rem = jnp.sum(c_rem * trace, axis=1, keepdims=True)
        norm = 1.0 / (jnp.sum(trace * trace, axis=1, keepdims=True) + EPS * frames)
        trace_bf = trace.astype(BF)
        sum_own = jnp.zeros((slots, LANES), F32)
        sum_rem = jnp.zeros((slots, LANES), F32)
        sum_sq = jnp.zeros((slots, LANES), F32)
        for first in range(0, pixels, WIDE):
            span = slice(first, first + WIDE)
            mine = a_own[:, span]
            theirs = a_rem[:, span]
            if t == 0:
                across = shape[:, span]
            else:
                across = dot(trace_bf, res_t[:, span]) + mine * with_own
            foot = jnp.maximum(across + theirs * with_rem, 0.0) * norm
            sum_own = sum_own + narrow(mine * foot)
            sum_rem = sum_rem + narrow(theirs * foot)
            sum_sq = sum_sq + narrow(foot * foot)
            feet[:, span] = foot.astype(BF)
        if t == ITERS - 1:
            for first in range(0, pixels, WIDE):
                wide[:, first:first + WIDE] = lax.dot_general(
                    border_hot, feet[:, first:first + WIDE], (((0,), (0,)), ((), ())), preferred_element_type=F32)
        down_sum = dot(feet[...], res_ref[...])
        if t == ITERS - 1:
            slid = {}
            for d in ORDER:
                emit(d, span1(d), False, slid)
        dot_own = jnp.sum(sum_own, axis=1, keepdims=True)
        dot_rem = jnp.sum(sum_rem, axis=1, keepdims=True)
        scale = 1.0 / (jnp.sum(sum_sq, axis=1, keepdims=True) + EPS * pixels)
        trace = jnp.maximum(down_sum + c_own * dot_own + c_rem * dot_rem, 0.0) * scale

    trace_bf = trace.astype(BF)
    sent = lax.dot_general(border_hot, trace_bf, (((0,), (0,)), ((), ())), preferred_element_type=F32)
    sent = jnp.where(hit, sent, -1.0)
    for d in range(8):
        first = span1(d) + lanes_in(d, pixels)[1]
        send[d, :, first:first + frames] = sent[PAD * d:PAD * d + PAD].astype(BF)
    issue(both)

    upper = slice(nb, comps)
    hot_up = own_hot[:, upper]
    ones = jnp.ones((slots, 128), BF)
    hit_up = lax.dot_general(hot_up, ones, (((0,), (0,)), ((), ())), preferred_element_type=F32)[:, 0:1] > 0.5
    alive_up = alive[upper]
    for first in range(0, pixels, CHUNK):
        span = slice(first, first + CHUNK)
        new = lax.dot_general(hot_up, feet[:, span], (((0,), (0,)), ((), ())), preferred_element_type=F32)
        new = jnp.where(hit_up, new, foot_ref[upper, span].astype(F32))
        out_foot[upper, span] = jnp.where(alive_up, new, 0.0).astype(BF)
    new = lax.dot_general(hot_up, trace_bf, (((0,), (0,)), ((), ())), preferred_element_type=F32)
    new = jnp.where(hit_up, new, own_traces[upper].astype(F32))
    out_trace[upper, :] = jnp.where(alive_up, new, 0.0).astype(BF)

    local = own_traces.astype(F32)
    local = local - jnp.mean(local, axis=1, keepdims=True)
    remote_traces = dot(squeeze, border_trace[...])
    remote_traces = remote_traces - jnp.mean(remote_traces, axis=1, keepdims=True)
    spread_remote = jnp.mean(remote_traces * remote_traces, axis=1, keepdims=True)
    full = functools.partial(lax.dot_general, dimension_numbers=(((1,), (1,)), ((), ())),
                             precision=lax.Precision.HIGHEST, preferred_element_type=F32)
    cov = full(remote_traces, local) / frames
    spread_local = full(jnp.ones((8, frames), F32), local * local)[0:1] / frames
    corr = cov / jnp.sqrt((spread_local + EPS) * (spread_remote + EPS))
    out_corr[...] = jnp.where(iota((1, comps), 1) < comp_count[0, 0], corr, 0.0)

    for first in range(0, pixels, CHUNK):
        span = slice(first, first + CHUNK)
        final[:, span] = foot_ref[0:nb, span].astype(F32)
    final_trace[...] = own_traces[0:nb].astype(F32)
    for d in RECEIVE:
        start, width = lanes_out(d, pixels)
        oy, ox = offsets(d)
        part = slice(NBR * d, NBR * d + NBR)

        @pl.when(exists(d))
        def _():
            both(7 - d).wait_recv()
            new = recv2[d, :, width:width + frames].astype(F32)[0:NBR]
            came = new >= 0.0
            final_trace[part, :] = jnp.where(came, new, final_trace[part, :])
            for first in range(0, width, LANES):
                span = slice(start + first, start + first + LANES)
                new = recv2[d, :, first:first + LANES].astype(F32)[0:NBR]
                final[part, span] = jnp.where(came & inside_of(oy, ox, start + first, LANES), new, final[part, span])

    out_trace[0:nb, :] = jnp.where(alive_low, final_trace[...], 0.0).astype(BF)
    for first in range(0, pixels, CHUNK):
        span = slice(first, first + CHUNK)
        out_foot[0:nb, span] = jnp.where(alive_low, final[:, span], 0.0).astype(BF)

    for d in range(8):
        @pl.when(exists(d))
        def _():
            all_sent(d).wait_send()


def store(foot, trace, corr, out_foot, out_trace, out_corr, sem):
    pairs = ((foot, out_foot), (trace, out_trace), (corr, out_corr))
    copies = [pltpu.make_async_copy(a, b, sem.at[i]) for i, (a, b) in enumerate(pairs)]
    for copy in copies:
        copy.start()
    for copy in copies:
        copy.wait()


def shards(rows, cols, residual, footprints, traces, merge_pairs, pair_counts, comp_counts, row_int, col_int):
    pixels, frames = residual.shape[2:]
    comps = footprints.shape[2]
    slots = merge_pairs.shape[2]
    nb, nbp = 8 * NBR, 8 * PAD
    vmem = pl.BlockSpec(memory_space=pltpu.VMEM)
    smem = pl.BlockSpec(memory_space=pltpu.SMEM)
    hbm = pl.BlockSpec(memory_space=pltpu.HBM)
    i32 = jnp.int32
    both = pltpu.VMEM((8, PAD, pixels + frames), BF)
    pairs = jnp.transpose(merge_pairs, (0, 3, 1, 2))[0]
    out_shape = (
        jax.ShapeDtypeStruct((comps, pixels), BF),
        jax.ShapeDtypeStruct((comps, frames), BF),
        jax.ShapeDtypeStruct((nb, comps), F32),
    )
    results = pl.pallas_call(
        functools.partial(kernel, rows, cols),
        out_shape=out_shape,
        in_specs=[hbm] * 4 + [smem] * 2 + [hbm] * 2,
        out_specs=(vmem,) * 3,
        scratch_shapes=[
            pltpu.VMEM((pixels, frames), BF), pltpu.VMEM((comps, pixels), BF), pltpu.VMEM((comps, frames), BF),
            pltpu.VMEM((3, 1, slots), i32),
            pltpu.SMEM(row_int.shape, i32), pltpu.SMEM(col_int.shape, i32),
            pltpu.VMEM((8, PAD, 2 * (pixels + frames)), BF), both, both,
            pltpu.VMEM((nbp, pixels), F32), pltpu.VMEM((frames, pixels), BF),
            pltpu.VMEM((nbp, pixels), BF), pltpu.VMEM((nbp, frames), BF),
            pltpu.VMEM((slots, pixels), F32), pltpu.VMEM((slots, pixels), F32),
            pltpu.VMEM((slots, pixels), F32), pltpu.VMEM((slots, pixels), BF),
            pltpu.VMEM((nb, pixels), F32), pltpu.VMEM((nb, frames), F32),
            pltpu.SemaphoreType.DMA((8,)), pltpu.SemaphoreType.DMA((2, 8)),
        ],
        compiler_params=pltpu.CompilerParams(
            collective_id=0, has_side_effects=True, vmem_limit_bytes=32 * 1024 * 1024),
    )(*[pltpu.with_memory_space_constraint(x, pltpu.HBM) for x in (
        residual[0, 0], footprints[0, 0], traces[0, 0], pairs)], pair_counts, comp_counts,
      *[pltpu.with_memory_space_constraint(x, pltpu.HBM) for x in (row_int, col_int)])
    foot, trace, corr = pl.pallas_call(
        store,
        out_shape=out_shape,
        in_specs=[vmem] * 3,
        out_specs=(hbm,) * 3,
        scratch_shapes=[pltpu.SemaphoreType.DMA((3,))],
        compiler_params=pltpu.CompilerParams(vmem_limit_bytes=4 * 1024 * 1024),
    )(*results)
    return foot[None, None], trace[None, None], jnp.transpose(corr)[None, None]


def solution(mesh):
    rows, cols = mesh.shape["py"], mesh.shape["px"]
    spec = P("py", "px", None, None)
    return jax.shard_map(
        functools.partial(shards, rows, cols), mesh=mesh,
        in_specs=(spec, spec, spec, spec, P("py", "px"), P("py", "px"), P(), P()),
        out_specs=(spec, spec, spec), check_vma=False)
```

```python
import functools

import jax
import jax.numpy as jnp
from jax import lax
from jax.experimental import pallas as pl
from jax.experimental.pallas import tpu as pltpu
from jax.sharding import PartitionSpec as P

PH = 64
PW = 64
NBR = 3
OV_HI = 24
ITERS = 4
EPS = 1e-05

PAD = 4
STRIP = OV_HI * PW
CHUNK = 512
WIDE = 1024
LANES = 128
LOW = (PH - OV_HI) // 2
ORDER = (0, 2, 5, 7, 1, 6, 3, 4)
RECEIVE = (3, 4, 1, 6, 0, 2, 5, 7)
STEPS = [(-1, -1), (-1, 0), (-1, 1), (0, -1), (0, 1), (1, -1), (1, 0), (1, 1)]
BF = jnp.bfloat16
F32 = jnp.float32
MESH = pl.DeviceIdType.MESH


def lanes_in(direction, pixels):
    dy = STEPS[direction][0]
    if dy > 0:
        return (0, STRIP)
    if dy < 0:
        return (pixels - STRIP, STRIP)
    return (0, pixels)


def lanes_out(direction, pixels):
    return lanes_in(7 - direction, pixels)


def dot(a, b):
    return jnp.dot(a, b, preferred_element_type=F32)


def dot_t(a, b):
    return lax.dot_general(a, b, (((1,), (1,)), ((), ())), preferred_element_type=F32)


def iota(shape, dim):
    return lax.broadcasted_iota(jnp.int32, shape, dim)


def narrow(x):
    return functools.reduce(jnp.add, [x[:, b:b + LANES] for b in range(0, x.shape[1], LANES)])


def inside_of(oy, ox, first, count):
    pixel = iota((1, count), 1) + first
    y = (pixel >> 6) - oy
    x = (pixel & (PW - 1)) - ox
    return (y >= 0) & (y < PH) & (x >= 0) & (x < PW)


def kernel(
    rows, cols,
    res_hbm, foot_hbm, trace_hbm, pair_hbm, pair_count, comp_count, row_hbm, col_hbm,
    out_foot, out_trace, out_corr,
    res_ref, foot_ref, trace_ref, pair_ref, row_ref, col_ref,
    send, recv1, recv2, wide, res_t,
    border_trace, c_rem_ref, a_own, a_rem, shape, feet, final, final_trace,
    sem_s, sem_r,
):
    pixels = foot_ref.shape[1]
    frames = trace_ref.shape[1]
    comps = foot_ref.shape[0]
    slots = pair_ref.shape[2]
    nb = 8 * NBR
    nbp = 8 * PAD
    my_r = lax.axis_index("py")
    my_c = lax.axis_index("px")

    def target(d):
        return (my_r + STEPS[d][0], my_c + STEPS[d][1])

    def exists(d):
        r, c = target(d)
        return (r >= 0) & (r < rows) & (c >= 0) & (c < cols)

    barrier = pltpu.get_barrier_semaphore()
    for d in ORDER:
        @pl.when(exists(d))
        def _():
            pl.semaphore_signal(barrier, 1, device_id=target(d), device_id_type=MESH)
    fetches = [
        (trace_hbm, trace_ref),
        (row_hbm, row_ref), (col_hbm, col_ref),
        (foot_hbm.at[pl.ds(0, nb)], foot_ref.at[pl.ds(0, nb)]),
        (pair_hbm, pair_ref),
        (foot_hbm.at[pl.ds(nb, comps - nb)], foot_ref.at[pl.ds(nb, comps - nb)]),
        (res_hbm, res_ref),
    ]
    fetches = [pltpu.make_async_copy(a, b, sem_s.at[i]) for i, (a, b) in enumerate(fetches)]
    for fetch in fetches:
        fetch.start()

    def span1(d):
        return lanes_in(d, pixels)[1] + frames

    def remote(src, dst, d, phase):
        return pltpu.make_async_remote_copy(
            src, dst, sem_s.at[d], sem_r.at[phase, 7 - d],
            device_id=target(d), device_id_type=MESH)

    def copy1(d):
        part = pl.ds(0, span1(d))
        return remote(send.at[d, :, part], recv1.at[7 - d, :, part], d, 0)

    def both(d):
        part = pl.ds(0, span1(d))
        return remote(send.at[d, :, pl.ds(span1(d), span1(d))], recv2.at[7 - d, :, part], d, 1)

    def issue(copy):
        odd = (my_c & 1) == 1
        for d, when in ((2, odd), (7, odd), (0, None), (5, None), (2, ~odd), (7, ~odd), (1, None), (6, None), (3, None), (4, None)):
            @pl.when(exists(d) if when is None else exists(d) & when)
            def _():
                copy(d).start()

    def all_sent(d):
        part = send.at[d, :, pl.ds(0, 2 * span1(d))]
        return remote(part, part, d, 1)

    j = iota((nbp, nb), 0)
    pick = (((j & (PAD - 1)) < NBR) & (iota((nbp, nb), 1) == NBR * (j >> 2) + (j & (PAD - 1)))).astype(BF)
    a_rem[...] = jnp.zeros_like(a_rem)
    c_rem_ref[...] = jnp.zeros_like(c_rem_ref)
    border_trace[...] = jnp.zeros_like(border_trace)
    fetches[0].wait()
    own_traces = trace_ref[...]
    packed_traces = dot(pick, own_traces[0:nb])
    for d in range(8):
        width = lanes_in(d, pixels)[1]
        send[d, :, width:width + frames] = packed_traces[PAD * d:PAD * d + PAD].astype(BF)
    fetches[1].wait()
    fetches[2].wait()
    up = row_ref[jnp.clip(my_r - 1, 0, rows - 2)]
    down = row_ref[jnp.clip(my_r, 0, rows - 2)]
    left = col_ref[jnp.clip(my_c - 1, 0, cols - 2)]
    right = col_ref[jnp.clip(my_c, 0, cols - 2)]

    def offsets(d):
        dy, dx = STEPS[d]
        oy = up - PH if dy < 0 else PH - down if dy > 0 else 0
        ox = left - PW if dx < 0 else PW - right if dx > 0 else 0
        return oy, ox

    def slide(part, dy):
        count = STRIP // LANES
        base = (pixels - STRIP) if dy > 0 else 0
        oy = offsets(6 if dy > 0 else 1)[0]
        steps = (oy >> 1) - LOW if dy > 0 else 0 - LOW - (oy >> 1)
        stack = jnp.concatenate([wide[part, base + LANES * b:base + LANES * (b + 1)] for b in range(count)], axis=0)
        stack = jnp.concatenate([stack, stack[8 * (count - 1):]], axis=0)
        for bit in (3, 2, 1, 0):
            jump = 8 << bit
            chosen = jnp.broadcast_to(((steps >> bit) & 1) == 1, (8 * count + 8 - jump, LANES))
            if dy > 0:
                moved = jnp.where(chosen, stack[jump:], stack[:-jump])
                stack = jnp.concatenate([moved, stack[-jump:]], axis=0)
            else:
                moved = jnp.where(chosen, stack[:-jump], stack[jump:])
                stack = jnp.concatenate([stack[:jump], moved], axis=0)
        return stack

    def emit(d, first, masked, slid):
        oy, ox = offsets(d)
        dy, dx = STEPS[d]
        start, width = lanes_in(d, pixels)
        blocks = width // LANES
        part = slice(8 * (d // 2), 8 * (d // 2) + 8)
        low = PAD * (d % 2)
        if dy == 0:
            stack = jnp.concatenate([wide[part, LANES * b:LANES * (b + 1)] for b in range(blocks)], axis=0)
            stack = pltpu.roll(stack, (0 - ox) & (LANES - 1), 1)
        else:
            if (d // 2, dy) not in slid:
                slid[d // 2, dy] = slide(part, dy)
            odd = oy & 1
            stack = pltpu.roll(slid[d // 2, dy], (0 - ox - PW * odd) & (LANES - 1), 1)
            later = (iota((8 * blocks, LANES), 1) >= PW * (2 - odd))
            stack = jnp.where(later, stack[8:], stack[:-8])
        if masked:
            lane = iota((8 * blocks, LANES), 1)
            y = (start >> 6) + 2 * (iota((8 * blocks, LANES), 0) >> 3) + (lane >> 6) + oy
            x = (lane & (PW - 1)) + ox
            stack = jnp.where((y >= 0) & (y < PH) & (x >= 0) & (x < PW), stack, 0.0)
        for b in range(blocks):
            send[d, :, first + LANES * b:first + LANES * (b + 1)] = stack[8 * b + low:8 * b + low + PAD].astype(BF)

    fetches[3].wait()
    for first in range(0, pixels, CHUNK):
        wide[:, first:first + CHUNK] = dot(pick, foot_ref[0:nb, first:first + CHUNK])
    slid = {}
    for d in ORDER:
        emit(d, 0, True, slid)

    for fetch in fetches[4:]:
        fetch.wait()
    total = jnp.int32(0)
    for d in range(8):
        total = total + exists(d).astype(jnp.int32)
    pl.semaphore_wait(barrier, total)
    issue(copy1)

    same = iota((slots, slots), 0) == iota((slots, slots), 1)

    def column(values):
        grid = jnp.where(same, values.astype(F32), 0.0)
        return jnp.sum(grid, axis=1, keepdims=True).astype(jnp.int32)

    ids = column(pair_ref[0])
    direction = column(pair_ref[1])
    place = column(pair_ref[2])
    live = iota((slots, 1), 0) < pair_count[0, 0]
    own_hot = ((iota((slots, comps), 1) == ids) & live).astype(BF)
    border_slot = PAD * direction + place
    border_hot = ((iota((slots, nbp), 1) == border_slot) & live).astype(BF)
    hit = lax.dot_general(border_hot, jnp.ones((slots, LANES), BF), (((0,), (0,)), ((), ())),
                          preferred_element_type=F32) > 0.5
    slot_of = lax.dot_general(border_hot, iota((slots, LANES), 0).astype(BF), (((0,), (0,)), ((), ())),
                              preferred_element_type=F32).astype(jnp.int32)

    c_own = dot(own_hot, own_traces)
    c_own_bf = c_own.astype(BF)
    energy = jnp.sum(c_own * c_own, axis=1, keepdims=True)
    for first in range(0, pixels, CHUNK):
        span = slice(first, first + CHUNK)
        mine = dot(own_hot, foot_ref[:, span])
        a_own[:, span] = mine
        turned = jnp.transpose(res_ref[span, :])
        res_t[:, span] = turned
        shape[:, span] = dot(c_own_bf, turned) + mine * energy

    k = iota((nb, nbp), 0)
    dir_wide = jnp.zeros((nb, nbp), jnp.int32)
    for d in range(1, 8):
        dir_wide = dir_wide + (k >= NBR * d).astype(jnp.int32)
    squeeze = (iota((nb, nbp), 1) == PAD * dir_wide + k - NBR * dir_wide).astype(BF)
    alive = iota((comps, 1), 0) < comp_count[0, 0]
    alive_low = alive[0:nb]

    place_wide = jnp.broadcast_to(place & (PAD - 1), (slots, LANES))
    direction_wide = jnp.broadcast_to(jnp.where(live, direction, -1), (slots, LANES))

    def gather(d, first, to, span):
        got = recv1[d, :, first:first + LANES].astype(F32)
        got = jnp.concatenate([got, got], axis=0)
        for low in range(0, slots, 8):
            part = slice(low, low + 8)
            row = jnp.take_along_axis(got, place_wide[part], axis=0)
            to[part, span] = jnp.where(direction_wide[part] == d, row, to[part, span])

    for d in RECEIVE:
        start, width = lanes_out(d, pixels)

        @pl.when(exists(d))
        def _():
            copy1(7 - d).wait_recv()
            gather(d, width, c_rem_ref, slice(0, frames))
            for first in range(0, width, LANES):
                gather(d, first, a_rem, slice(start + first, start + first + LANES))
            border_trace[PAD * d:PAD * d + PAD, :] = recv1[d, :, width:width + frames]

    c_rem = c_rem_ref[...]

    def choose(values, low):
        at = slot_of[low:low + 8]
        row = jnp.take_along_axis(values[0:8], at & 7, axis=0)
        for first in range(8, slots, 8):
            row = jnp.where(at >= first, jnp.take_along_axis(values[first:first + 8], at & 7, axis=0), row)
        return row

    trace = c_own
    for t in range(ITERS):
        with_own = jnp.sum(c_own * trace, axis=1, keepdims=True)
        with_rem = jnp.sum(c_rem * trace, axis=1, keepdims=True)
        norm = 1.0 / (jnp.sum(trace * trace, axis=1, keepdims=True) + EPS * frames)
        trace_bf = trace.astype(BF)
        sum_own = jnp.zeros((slots, LANES), F32)
        sum_rem = jnp.zeros((slots, LANES), F32)
        sum_sq = jnp.zeros((slots, LANES), F32)
        for first in range(0, pixels, WIDE):
            span = slice(first, first + WIDE)
            mine = a_own[:, span]
            theirs = a_rem[:, span]
            if t == 0:
                across = shape[:, span]
            else:
                across = dot(trace_bf, res_t[:, span]) + mine * with_own
            foot = jnp.maximum(across + theirs * with_rem, 0.0) * norm
            sum_own = sum_own + narrow(mine * foot)
            sum_rem = sum_rem + narrow(theirs * foot)
            sum_sq = sum_sq + narrow(foot * foot)
            feet[:, span] = foot.astype(BF)
        if t == ITERS - 1:
            for low in range(0, nbp, 8):
                rows_of = [STEPS[d][0] for d in (low // PAD, low // PAD + 1)]
                begin = 0 if min(rows_of) <= 0 else pixels - STRIP
                end = pixels if max(rows_of) >= 0 else STRIP
                for first in range(begin, end, LANES):
                    span = slice(first, first + LANES)
                    wide[low:low + 8, span] = choose(feet[:, span].astype(F32), low)
        down_sum = dot(feet[...], res_ref[...])
        if t == ITERS - 1:
            slid = {}
            for d in ORDER:
                emit(d, span1(d), False, slid)
        dot_own = jnp.sum(sum_own, axis=1, keepdims=True)
        dot_rem = jnp.sum(sum_rem, axis=1, keepdims=True)
        scale = 1.0 / (jnp.sum(sum_sq, axis=1, keepdims=True) + EPS * pixels)
        trace = jnp.maximum(down_sum + c_own * dot_own + c_rem * dot_rem, 0.0) * scale

    trace_bf = trace.astype(BF)
    sent = jnp.where(hit, jnp.concatenate([choose(trace, low) for low in range(0, nbp, 8)], axis=0), -1.0)
    for d in range(8):
        first = span1(d) + lanes_in(d, pixels)[1]
        send[d, :, first:first + frames] = sent[PAD * d:PAD * d + PAD].astype(BF)
    issue(both)

    upper = slice(nb, comps)
    hot_up = own_hot[:, upper]
    ones = jnp.ones((slots, 128), BF)
    hit_up = lax.dot_general(hot_up, ones, (((0,), (0,)), ((), ())), preferred_element_type=F32)[:, 0:1] > 0.5
    alive_up = alive[upper]
    for first in range(0, pixels, CHUNK):
        span = slice(first, first + CHUNK)
        new = lax.dot_general(hot_up, feet[:, span], (((0,), (0,)), ((), ())), preferred_element_type=F32)
        new = jnp.where(hit_up, new, foot_ref[upper, span].astype(F32))
        out_foot[upper, span] = jnp.where(alive_up, new, 0.0).astype(BF)
    new = lax.dot_general(hot_up, trace_bf, (((0,), (0,)), ((), ())), preferred_element_type=F32)
    new = jnp.where(hit_up, new, own_traces[upper].astype(F32))
    out_trace[upper, :] = jnp.where(alive_up, new, 0.0).astype(BF)

    local = own_traces.astype(F32)
    local = local - jnp.mean(local, axis=1, keepdims=True)
    remote_traces = dot(squeeze, border_trace[...])
    remote_traces = remote_traces - jnp.mean(remote_traces, axis=1, keepdims=True)
    spread_remote = jnp.mean(remote_traces * remote_traces, axis=1, keepdims=True)
    full = functools.partial(lax.dot_general, dimension_numbers=(((1,), (1,)), ((), ())),
                             precision=lax.Precision.HIGHEST, preferred_element_type=F32)
    cov = full(remote_traces, local) / frames
    spread_local = full(jnp.ones((8, frames), F32), local * local)[0:1] / frames
    corr = cov / jnp.sqrt((spread_local + EPS) * (spread_remote + EPS))
    out_corr[...] = jnp.where(iota((1, comps), 1) < comp_count[0, 0], corr, 0.0)

    for first in range(0, pixels, CHUNK):
        span = slice(first, first + CHUNK)
        final[:, span] = foot_ref[0:nb, span].astype(F32)
    final_trace[...] = own_traces[0:nb].astype(F32)
    for d in RECEIVE:
        start, width = lanes_out(d, pixels)
        oy, ox = offsets(d)
        part = slice(NBR * d, NBR * d + NBR)

        @pl.when(exists(d))
        def _():
            both(7 - d).wait_recv()
            new = recv2[d, :, width:width + frames].astype(F32)[0:NBR]
            came = new >= 0.0
            final_trace[part, :] = jnp.where(came, new, final_trace[part, :])
            for first in range(0, width, LANES):
                span = slice(start + first, start + first + LANES)
                new = recv2[d, :, first:first + LANES].astype(F32)[0:NBR]
                final[part, span] = jnp.where(came & inside_of(oy, ox, start + first, LANES), new, final[part, span])

    out_trace[0:nb, :] = jnp.where(alive_low, final_trace[...], 0.0).astype(BF)
    for first in range(0, pixels, CHUNK):
        span = slice(first, first + CHUNK)
        out_foot[0:nb, span] = jnp.where(alive_low, final[:, span], 0.0).astype(BF)

    for d in range(8):
        @pl.when(exists(d))
        def _():
            all_sent(d).wait_send()


def store(foot, trace, corr, out_foot, out_trace, out_corr, sem):
    pairs = ((foot, out_foot), (trace, out_trace), (corr, out_corr))
    copies = [pltpu.make_async_copy(a, b, sem.at[i]) for i, (a, b) in enumerate(pairs)]
    for copy in copies:
        copy.start()
    for copy in copies:
        copy.wait()


def shards(rows, cols, residual, footprints, traces, merge_pairs, pair_counts, comp_counts, row_int, col_int):
    pixels, frames = residual.shape[2:]
    comps = footprints.shape[2]
    slots = merge_pairs.shape[2]
    nb, nbp = 8 * NBR, 8 * PAD
    vmem = pl.BlockSpec(memory_space=pltpu.VMEM)
    smem = pl.BlockSpec(memory_space=pltpu.SMEM)
    hbm = pl.BlockSpec(memory_space=pltpu.HBM)
    i32 = jnp.int32
    both = pltpu.VMEM((8, PAD, pixels + frames), BF)
    pairs = jnp.transpose(merge_pairs, (0, 3, 1, 2))[0]
    out_shape = (
        jax.ShapeDtypeStruct((comps, pixels), BF),
        jax.ShapeDtypeStruct((comps, frames), BF),
        jax.ShapeDtypeStruct((nb, comps), F32),
    )
    results = pl.pallas_call(
        functools.partial(kernel, rows, cols),
        out_shape=out_shape,
        in_specs=[hbm] * 4 + [smem] * 2 + [hbm] * 2,
        out_specs=(vmem,) * 3,
        scratch_shapes=[
            pltpu.VMEM((pixels, frames), BF), pltpu.VMEM((comps, pixels), BF), pltpu.VMEM((comps, frames), BF),
            pltpu.VMEM((3, 1, slots), i32),
            pltpu.SMEM(row_int.shape, i32), pltpu.SMEM(col_int.shape, i32),
            pltpu.VMEM((8, PAD, 2 * (pixels + frames)), BF), both, both,
            pltpu.VMEM((nbp, pixels), F32), pltpu.VMEM((frames, pixels), BF),
            pltpu.VMEM((nbp, frames), BF), pltpu.VMEM((slots, frames), F32),
            pltpu.VMEM((slots, pixels), F32), pltpu.VMEM((slots, pixels), F32),
            pltpu.VMEM((slots, pixels), F32), pltpu.VMEM((slots, pixels), BF),
            pltpu.VMEM((nb, pixels), F32), pltpu.VMEM((nb, frames), F32),
            pltpu.SemaphoreType.DMA((8,)), pltpu.SemaphoreType.DMA((2, 8)),
        ],
        compiler_params=pltpu.CompilerParams(
            collective_id=0, has_side_effects=True, vmem_limit_bytes=32 * 1024 * 1024),
    )(*[pltpu.with_memory_space_constraint(x, pltpu.HBM) for x in (
        residual[0, 0], footprints[0, 0], traces[0, 0], pairs)], pair_counts, comp_counts,
      *[pltpu.with_memory_space_constraint(x, pltpu.HBM) for x in (row_int, col_int)])
    foot, trace, corr = pl.pallas_call(
        store,
        out_shape=out_shape,
        in_specs=[vmem] * 3,
        out_specs=(hbm,) * 3,
        scratch_shapes=[pltpu.SemaphoreType.DMA((3,))],
        compiler_params=pltpu.CompilerParams(vmem_limit_bytes=4 * 1024 * 1024),
    )(*results)
    return foot[None, None], trace[None, None], jnp.transpose(corr)[None, None]


def solution(mesh):
    rows, cols = mesh.shape["py"], mesh.shape["px"]
    spec = P("py", "px", None, None)
    return jax.shard_map(
        functools.partial(shards, rows, cols), mesh=mesh,
        in_specs=(spec, spec, spec, spec, P("py", "px"), P("py", "px"), P(), P()),
        out_specs=(spec, spec, spec), check_vma=False)
```

```python
import functools

import jax
import jax.numpy as jnp
from jax import lax
from jax.experimental import pallas as pl
from jax.experimental.pallas import tpu as pltpu
from jax.sharding import PartitionSpec as P

PH = 64
PW = 64
NBR = 3
OV_HI = 24
ITERS = 4
EPS = 1e-05

PAD = 4
STRIP = OV_HI * PW
CHUNK = 512
WIDE = 1024
LANES = 128
LOW = (PH - OV_HI) // 2
ORDER = (0, 2, 5, 7, 1, 6, 3, 4)
ISSUE = ((2, 1), (7, 1), (0, None), (5, None), (2, 0), (7, 0), (1, None), (6, None), (3, None), (4, None))
RECEIVE = ((3, None), (4, None), (1, None), (6, None), (0, 1), (5, 1), (2, 0), (7, 0), (0, 0), (5, 0), (2, 1), (7, 1))
STEPS = [(-1, -1), (-1, 0), (-1, 1), (0, -1), (0, 1), (1, -1), (1, 0), (1, 1)]
BF = jnp.bfloat16
F32 = jnp.float32
MESH = pl.DeviceIdType.MESH


def lanes_in(direction, pixels):
    dy = STEPS[direction][0]
    if dy > 0:
        return (0, STRIP)
    if dy < 0:
        return (pixels - STRIP, STRIP)
    return (0, pixels)


def lanes_out(direction, pixels):
    return lanes_in(7 - direction, pixels)


def dot(a, b):
    return jnp.dot(a, b, preferred_element_type=F32)


def dot_t(a, b):
    return lax.dot_general(a, b, (((1,), (1,)), ((), ())), preferred_element_type=F32)


def iota(shape, dim):
    return lax.broadcasted_iota(jnp.int32, shape, dim)


def narrow(x):
    return functools.reduce(jnp.add, [x[:, b:b + LANES] for b in range(0, x.shape[1], LANES)])


def inside_of(oy, ox, first, count):
    pixel = iota((1, count), 1) + first
    y = (pixel >> 6) - oy
    x = (pixel & (PW - 1)) - ox
    return (y >= 0) & (y < PH) & (x >= 0) & (x < PW)


def kernel(
    rows, cols,
    res_hbm, foot_hbm, trace_hbm, pair_hbm, pair_count, comp_count, row_hbm, col_hbm,
    out_foot, out_trace, out_corr,
    res_ref, foot_ref, trace_ref, pair_ref, row_ref, col_ref,
    send, recv1, recv2, wide, res_t,
    border_trace, c_rem_ref, a_own, a_rem, shape, feet, final, final_trace,
    sem_s, sem_r, sem_f,
):
    pixels = foot_ref.shape[1]
    frames = trace_ref.shape[1]
    comps = foot_ref.shape[0]
    slots = pair_ref.shape[2]
    nb = 8 * NBR
    nbp = 8 * PAD
    my_r = lax.axis_index("py")
    my_c = lax.axis_index("px")

    def target(d):
        return (my_r + STEPS[d][0], my_c + STEPS[d][1])

    def exists(d):
        r, c = target(d)
        return (r >= 0) & (r < rows) & (c >= 0) & (c < cols)

    def now(d, parity):
        return exists(d) if parity is None else exists(d) & ((my_c & 1) == parity)

    barrier = pltpu.get_barrier_semaphore()
    for d, parity in ISSUE:
        @pl.when(now(d, parity))
        def _():
            pl.semaphore_signal(barrier, 1, device_id=target(d), device_id_type=MESH)
    fetches = [
        (trace_hbm, trace_ref),
        (row_hbm, row_ref), (col_hbm, col_ref),
        (foot_hbm.at[pl.ds(0, nb)], foot_ref.at[pl.ds(0, nb)]),
        (pair_hbm, pair_ref),
        (foot_hbm.at[pl.ds(nb, comps - nb)], foot_ref.at[pl.ds(nb, comps - nb)]),
        (res_hbm, res_ref),
    ]
    fetches = [pltpu.make_async_copy(a, b, sem_s.at[i] if i < 6 else sem_f.at[0]) for i, (a, b) in enumerate(fetches)]
    for fetch in fetches:
        fetch.start()

    def span1(d):
        return lanes_in(d, pixels)[1] + frames

    def remote(src, dst, d, phase):
        return pltpu.make_async_remote_copy(
            src, dst, sem_s.at[d], sem_r.at[phase, 7 - d],
            device_id=target(d), device_id_type=MESH)

    def copy1(d):
        part = pl.ds(0, span1(d))
        return remote(send.at[d, :, part], recv1.at[7 - d, :, part], d, 0)

    def both(d):
        part = pl.ds(0, span1(d))
        return remote(send.at[d, :, pl.ds(span1(d), span1(d))], recv2.at[7 - d, :, part], d, 1)

    def issue(copy):
        for d, parity in ISSUE:
            @pl.when(now(d, parity))
            def _():
                copy(d).start()

    def all_sent(d):
        part = send.at[d, :, pl.ds(0, 2 * span1(d))]
        return remote(part, part, d, 1)

    j = iota((nbp, nb), 0)
    pick = (((j & (PAD - 1)) < NBR) & (iota((nbp, nb), 1) == NBR * (j >> 2) + (j & (PAD - 1)))).astype(BF)
    a_rem[...] = jnp.zeros_like(a_rem)
    c_rem_ref[...] = jnp.zeros_like(c_rem_ref)
    border_trace[...] = jnp.zeros_like(border_trace)
    fetches[0].wait()
    own_traces = trace_ref[...]
    packed_traces = dot(pick, own_traces[0:nb])
    for d in range(8):
        width = lanes_in(d, pixels)[1]
        send[d, :, width:width + frames] = packed_traces[PAD * d:PAD * d + PAD].astype(BF)
    fetches[1].wait()
    fetches[2].wait()
    up = row_ref[jnp.clip(my_r - 1, 0, rows - 2)]
    down = row_ref[jnp.clip(my_r, 0, rows - 2)]
    left = col_ref[jnp.clip(my_c - 1, 0, cols - 2)]
    right = col_ref[jnp.clip(my_c, 0, cols - 2)]

    def offsets(d):
        dy, dx = STEPS[d]
        oy = up - PH if dy < 0 else PH - down if dy > 0 else 0
        ox = left - PW if dx < 0 else PW - right if dx > 0 else 0
        return oy, ox

    def slide(part, dy):
        count = STRIP // LANES
        base = (pixels - STRIP) if dy > 0 else 0
        oy = offsets(6 if dy > 0 else 1)[0]
        steps = (oy >> 1) - LOW if dy > 0 else 0 - LOW - (oy >> 1)
        stack = jnp.concatenate([wide[part, base + LANES * b:base + LANES * (b + 1)] for b in range(count)], axis=0)
        stack = jnp.concatenate([stack, stack[8 * (count - 1):]], axis=0)
        for bit in (3, 2, 1, 0):
            jump = 8 << bit
            chosen = jnp.broadcast_to(((steps >> bit) & 1) == 1, (8 * count + 8 - jump, LANES))
            if dy > 0:
                moved = jnp.where(chosen, stack[jump:], stack[:-jump])
                stack = jnp.concatenate([moved, stack[-jump:]], axis=0)
            else:
                moved = jnp.where(chosen, stack[:-jump], stack[jump:])
                stack = jnp.concatenate([stack[:jump], moved], axis=0)
        return stack

    def emit(d, first, masked, slid):
        oy, ox = offsets(d)
        dy, dx = STEPS[d]
        start, width = lanes_in(d, pixels)
        blocks = width // LANES
        part = slice(8 * (d // 2), 8 * (d // 2) + 8)
        low = PAD * (d % 2)
        if dy == 0:
            stack = jnp.concatenate([wide[part, LANES * b:LANES * (b + 1)] for b in range(blocks)], axis=0)
            stack = pltpu.roll(stack, (0 - ox) & (LANES - 1), 1)
        else:
            if (d // 2, dy) not in slid:
                slid[d // 2, dy] = slide(part, dy)
            odd = oy & 1
            stack = pltpu.roll(slid[d // 2, dy], (0 - ox - PW * odd) & (LANES - 1), 1)
            later = (iota((8 * blocks, LANES), 1) >= PW * (2 - odd))
            stack = jnp.where(later, stack[8:], stack[:-8])
        if masked:
            lane = iota((8 * blocks, LANES), 1)
            y = (start >> 6) + 2 * (iota((8 * blocks, LANES), 0) >> 3) + (lane >> 6) + oy
            x = (lane & (PW - 1)) + ox
            stack = jnp.where((y >= 0) & (y < PH) & (x >= 0) & (x < PW), stack, 0.0)
        for b in range(blocks):
            send[d, :, first + LANES * b:first + LANES * (b + 1)] = stack[8 * b + low:8 * b + low + PAD].astype(BF)

    def pack(values, low):
        j = iota((8, LANES), 0)
        comp = (low // PAD) * NBR + NBR * (j >> 2) + jnp.minimum(j & (PAD - 1), NBR - 1)
        begin = (low // PAD) * NBR // 8 * 8
        row = jnp.take_along_axis(values[begin:begin + 8], comp & 7, axis=0)
        if begin + 8 < (low // PAD) * NBR + 2 * NBR:
            row = jnp.where(comp >= begin + 8, jnp.take_along_axis(values[begin + 8:begin + 16], comp & 7, axis=0), row)
        return row

    def spread(read, pick_rows):
        for low in range(0, nbp, 8):
            steps = [STEPS[d][0] for d in (low // PAD, low // PAD + 1)]
            begin = 0 if min(steps) <= 0 else pixels - STRIP
            end = pixels if max(steps) >= 0 else STRIP
            for first in range(begin, end, LANES):
                span = slice(first, first + LANES)
                wide[low:low + 8, span] = pick_rows(read(span), low)

    fetches[3].wait()
    spread(lambda span: foot_ref[0:nb, span].astype(F32), pack)
    slid = {}
    for d in ORDER:
        emit(d, 0, True, slid)

    for fetch in fetches[4:6]:
        fetch.wait()
    total = jnp.int32(0)
    for d in range(8):
        total = total + exists(d).astype(jnp.int32)
    pl.semaphore_wait(barrier, total)
    issue(copy1)

    same = iota((slots, slots), 0) == iota((slots, slots), 1)

    def column(values):
        grid = jnp.where(same, values.astype(F32), 0.0)
        return jnp.sum(grid, axis=1, keepdims=True).astype(jnp.int32)

    ids = column(pair_ref[0])
    direction = column(pair_ref[1])
    place = column(pair_ref[2])
    live = iota((slots, 1), 0) < pair_count[0, 0]
    own_hot = ((iota((slots, comps), 1) == ids) & live).astype(BF)
    border_slot = PAD * direction + place
    border_hot = ((iota((slots, nbp), 1) == border_slot) & live).astype(BF)
    hit = lax.dot_general(border_hot, jnp.ones((slots, LANES), BF), (((0,), (0,)), ((), ())),
                          preferred_element_type=F32) > 0.5
    slot_of = lax.dot_general(border_hot, iota((slots, LANES), 0).astype(BF), (((0,), (0,)), ((), ())),
                              preferred_element_type=F32).astype(jnp.int32)

    fetches[6].wait()
    c_own = dot(own_hot, own_traces)
    c_own_bf = c_own.astype(BF)
    energy = jnp.sum(c_own * c_own, axis=1, keepdims=True)
    for first in range(0, pixels, CHUNK):
        span = slice(first, first + CHUNK)
        mine = dot(own_hot, foot_ref[:, span])
        a_own[:, span] = mine
        turned = jnp.transpose(res_ref[span, :])
        res_t[:, span] = turned
        shape[:, span] = dot(c_own_bf, turned) + mine * energy

    k = iota((nb, nbp), 0)
    dir_wide = jnp.zeros((nb, nbp), jnp.int32)
    for d in range(1, 8):
        dir_wide = dir_wide + (k >= NBR * d).astype(jnp.int32)
    squeeze = (iota((nb, nbp), 1) == PAD * dir_wide + k - NBR * dir_wide).astype(BF)
    alive = iota((comps, 1), 0) < comp_count[0, 0]
    alive_low = alive[0:nb]

    place_wide = jnp.broadcast_to(place & (PAD - 1), (slots, LANES))
    direction_wide = jnp.broadcast_to(jnp.where(live, direction, -1), (slots, LANES))

    def gather(d, first, to, span):
        got = recv1[d, :, first:first + LANES].astype(F32)
        got = jnp.concatenate([got, got], axis=0)
        for low in range(0, slots, 8):
            part = slice(low, low + 8)
            row = jnp.take_along_axis(got, place_wide[part], axis=0)
            to[part, span] = jnp.where(direction_wide[part] == d, row, to[part, span])

    for d, parity in RECEIVE:
        start, width = lanes_out(d, pixels)

        @pl.when(now(d, parity))
        def _():
            copy1(7 - d).wait_recv()
            gather(d, width, c_rem_ref, slice(0, frames))
            for first in range(0, width, LANES):
                gather(d, first, a_rem, slice(start + first, start + first + LANES))
            border_trace[PAD * d:PAD * d + PAD, :] = recv1[d, :, width:width + frames]

    c_rem = c_rem_ref[...]

    def choose(values, low):
        at = slot_of[low:low + 8]
        row = jnp.take_along_axis(values[0:8], at & 7, axis=0)
        for first in range(8, slots, 8):
            row = jnp.where(at >= first, jnp.take_along_axis(values[first:first + 8], at & 7, axis=0), row)
        return row

    trace = c_own
    for t in range(ITERS):
        with_own = jnp.sum(c_own * trace, axis=1, keepdims=True)
        with_rem = jnp.sum(c_rem * trace, axis=1, keepdims=True)
        norm = 1.0 / (jnp.sum(trace * trace, axis=1, keepdims=True) + EPS * frames)
        trace_bf = trace.astype(BF)
        sum_own = jnp.zeros((slots, LANES), F32)
        sum_rem = jnp.zeros((slots, LANES), F32)
        sum_sq = jnp.zeros((slots, LANES), F32)
        for first in range(0, pixels, WIDE):
            span = slice(first, first + WIDE)
            mine = a_own[:, span]
            theirs = a_rem[:, span]
            if t == 0:
                across = shape[:, span]
            else:
                across = dot(trace_bf, res_t[:, span]) + mine * with_own
            foot = jnp.maximum(across + theirs * with_rem, 0.0) * norm
            sum_own = sum_own + narrow(mine * foot)
            sum_rem = sum_rem + narrow(theirs * foot)
            sum_sq = sum_sq + narrow(foot * foot)
            feet[:, span] = foot.astype(BF)
        if t == ITERS - 1:
            spread(lambda span: feet[:, span].astype(F32), choose)
        down_sum = dot(feet[...], res_ref[...])
        if t == ITERS - 1:
            slid = {}
            for d in ORDER:
                emit(d, span1(d), False, slid)
        dot_own = jnp.sum(sum_own, axis=1, keepdims=True)
        dot_rem = jnp.sum(sum_rem, axis=1, keepdims=True)
        scale = 1.0 / (jnp.sum(sum_sq, axis=1, keepdims=True) + EPS * pixels)
        trace = jnp.maximum(down_sum + c_own * dot_own + c_rem * dot_rem, 0.0) * scale

    trace_bf = trace.astype(BF)
    sent = jnp.where(hit, jnp.concatenate([choose(trace, low) for low in range(0, nbp, 8)], axis=0), -1.0)
    for d in range(8):
        first = span1(d) + lanes_in(d, pixels)[1]
        send[d, :, first:first + frames] = sent[PAD * d:PAD * d + PAD].astype(BF)
    issue(both)

    upper = slice(nb, comps)
    hot_up = own_hot[:, upper]
    ones = jnp.ones((slots, 128), BF)
    hit_up = lax.dot_general(hot_up, ones, (((0,), (0,)), ((), ())), preferred_element_type=F32)[:, 0:1] > 0.5
    alive_up = alive[upper]
    for first in range(0, pixels, CHUNK):
        span = slice(first, first + CHUNK)
        new = lax.dot_general(hot_up, feet[:, span], (((0,), (0,)), ((), ())), preferred_element_type=F32)
        new = jnp.where(hit_up, new, foot_ref[upper, span].astype(F32))
        out_foot[upper, span] = jnp.where(alive_up, new, 0.0).astype(BF)
    new = lax.dot_general(hot_up, trace_bf, (((0,), (0,)), ((), ())), preferred_element_type=F32)
    new = jnp.where(hit_up, new, own_traces[upper].astype(F32))
    out_trace[upper, :] = jnp.where(alive_up, new, 0.0).astype(BF)

    local = own_traces.astype(F32)
    local = local - jnp.mean(local, axis=1, keepdims=True)
    remote_traces = dot(squeeze, border_trace[...])
    remote_traces = remote_traces - jnp.mean(remote_traces, axis=1, keepdims=True)
    spread_remote = jnp.mean(remote_traces * remote_traces, axis=1, keepdims=True)
    full = functools.partial(lax.dot_general, dimension_numbers=(((1,), (1,)), ((), ())),
                             precision=lax.Precision.HIGHEST, preferred_element_type=F32)
    cov = full(remote_traces, local) / frames
    spread_local = full(jnp.ones((8, frames), F32), local * local)[0:1] / frames
    corr = cov / jnp.sqrt((spread_local + EPS) * (spread_remote + EPS))
    out_corr[...] = jnp.where(iota((1, comps), 1) < comp_count[0, 0], corr, 0.0)

    for first in range(0, pixels, CHUNK):
        span = slice(first, first + CHUNK)
        final[:, span] = foot_ref[0:nb, span].astype(F32)
    final_trace[...] = own_traces[0:nb].astype(F32)
    for d, parity in RECEIVE:
        start, width = lanes_out(d, pixels)
        oy, ox = offsets(d)
        part = slice(NBR * d, NBR * d + NBR)

        @pl.when(now(d, parity))
        def _():
            both(7 - d).wait_recv()
            new = recv2[d, :, width:width + frames].astype(F32)[0:NBR]
            came = new >= 0.0
            final_trace[part, :] = jnp.where(came, new, final_trace[part, :])
            for first in range(0, width, LANES):
                span = slice(start + first, start + first + LANES)
                new = recv2[d, :, first:first + LANES].astype(F32)[0:NBR]
                final[part, span] = jnp.where(came & inside_of(oy, ox, start + first, LANES), new, final[part, span])

    out_trace[0:nb, :] = jnp.where(alive_low, final_trace[...], 0.0).astype(BF)
    for first in range(0, pixels, CHUNK):
        span = slice(first, first + CHUNK)
        out_foot[0:nb, span] = jnp.where(alive_low, final[:, span], 0.0).astype(BF)

    for d in range(8):
        @pl.when(exists(d))
        def _():
            all_sent(d).wait_send()


def store(foot, trace, corr, out_foot, out_trace, out_corr, sem):
    pairs = ((foot, out_foot), (trace, out_trace), (corr, out_corr))
    copies = [pltpu.make_async_copy(a, b, sem.at[i]) for i, (a, b) in enumerate(pairs)]
    for copy in copies:
        copy.start()
    for copy in copies:
        copy.wait()


def shards(rows, cols, residual, footprints, traces, merge_pairs, pair_counts, comp_counts, row_int, col_int):
    pixels, frames = residual.shape[2:]
    comps = footprints.shape[2]
    slots = merge_pairs.shape[2]
    nb, nbp = 8 * NBR, 8 * PAD
    vmem = pl.BlockSpec(memory_space=pltpu.VMEM)
    smem = pl.BlockSpec(memory_space=pltpu.SMEM)
    hbm = pl.BlockSpec(memory_space=pltpu.HBM)
    i32 = jnp.int32
    both = pltpu.VMEM((8, PAD, pixels + frames), BF)
    pairs = jnp.transpose(merge_pairs, (0, 3, 1, 2))[0]
    out_shape = (
        jax.ShapeDtypeStruct((comps, pixels), BF),
        jax.ShapeDtypeStruct((comps, frames), BF),
        jax.ShapeDtypeStruct((nb, comps), F32),
    )
    results = pl.pallas_call(
        functools.partial(kernel, rows, cols),
        out_shape=out_shape,
        in_specs=[hbm] * 4 + [smem] * 2 + [hbm] * 2,
        out_specs=(vmem,) * 3,
        scratch_shapes=[
            pltpu.VMEM((pixels, frames), BF), pltpu.VMEM((comps, pixels), BF), pltpu.VMEM((comps, frames), BF),
            pltpu.VMEM((3, 1, slots), i32),
            pltpu.SMEM(row_int.shape, i32), pltpu.SMEM(col_int.shape, i32),
            pltpu.VMEM((8, PAD, 2 * (pixels + frames)), BF), both, both,
            pltpu.VMEM((nbp, pixels), F32), pltpu.VMEM((frames, pixels), BF),
            pltpu.VMEM((nbp, frames), BF), pltpu.VMEM((slots, frames), F32),
            pltpu.VMEM((slots, pixels), F32), pltpu.VMEM((slots, pixels), F32),
            pltpu.VMEM((slots, pixels), F32), pltpu.VMEM((slots, pixels), BF),
            pltpu.VMEM((nb, pixels), F32), pltpu.VMEM((nb, frames), F32),
            pltpu.SemaphoreType.DMA((8,)), pltpu.SemaphoreType.DMA((2, 8)), pltpu.SemaphoreType.DMA((1,)),
        ],
        compiler_params=pltpu.CompilerParams(
            collective_id=0, has_side_effects=True, vmem_limit_bytes=32 * 1024 * 1024),
    )(*[pltpu.with_memory_space_constraint(x, pltpu.HBM) for x in (
        residual[0, 0], footprints[0, 0], traces[0, 0], pairs)], pair_counts, comp_counts,
      *[pltpu.with_memory_space_constraint(x, pltpu.HBM) for x in (row_int, col_int)])
    foot, trace, corr = pl.pallas_call(
        store,
        out_shape=out_shape,
        in_specs=[vmem] * 3,
        out_specs=(hbm,) * 3,
        scratch_shapes=[pltpu.SemaphoreType.DMA((3,))],
        compiler_params=pltpu.CompilerParams(vmem_limit_bytes=4 * 1024 * 1024),
    )(*results)
    return foot[None, None], trace[None, None], jnp.transpose(corr)[None, None]


def solution(mesh):
    rows, cols = mesh.shape["py"], mesh.shape["px"]
    spec = P("py", "px", None, None)
    return jax.shard_map(
        functools.partial(shards, rows, cols), mesh=mesh,
        in_specs=(spec, spec, spec, spec, P("py", "px"), P("py", "px"), P(), P()),
        out_specs=(spec, spec, spec), check_vma=False)
```
